32 devices in a mesh: row: 4 (over z), col: 2 (over x), depth: 4 (over y, core).
Axes of the slice: x: 2, y: 2, z: 4, core: 2. Of those that a mesh axis runs over, the one named last changes fastest.
Arguments:
- eri_tiles: bfloat16 [48, 64, 128, 128], P('row', ('col', 'depth')), may hold values from -0.0625 to 0.0625
- screen: int32 [48, 64], P('row', ('col', 'depth')), may hold values from 0 to 1, as said below
- density_bra: bfloat16 [6144, 256], P('row', 'col'), may hold values from -6 to 6
- density_ket: bfloat16 [8192, 256], P(('col', 'depth'), 'row'), may hold values from -6 to 6
Outputs:
- coulomb_bra: float32 [6144, 256], P('row', 'col')
- coulomb_ket: float32 [8192, 256], P(('col', 'depth'), 'row')
The draws below stay inside these ranges and needn't reach their ends.
Inputs may be any that keep to these rules, and one draw needn't show every extreme that they name: `screen`: in each device's block of 12 x 8 tiles (aligned blocks), between 16 and 64 tiles are significant; some block has exactly 64.
All inputs are finite; a program needn't handle non-finite values.
Results may differ from the reference program's by a relative error of at most 0.005.
Values may be sent and summed in bfloat16 or wider, within the bound.
A program may use at most 64 MiB of HBM per device.

```python
import jax
import jax.numpy as jnp
from jax import lax

PAIR = 128
DENS = 256
A_DEV = 12
B_DEV = 8
NA = 48
NB = 64
CAP = 64


def draw_screen(key, part):
    blocks_r = NA // A_DEV
    blocks_c = NB // B_DEV
    tiles_dev = A_DEV * B_DEV
    devices_all = blocks_r * blocks_c
    lowest = max(1, CAP // 4)
    key_count, key_pick, key_perm = jax.random.split(jax.random.fold_in(key, 11), 3)
    counts = jax.random.randint(key_count, (devices_all,), lowest, CAP + 1)
    busiest = jax.random.randint(key_pick, (), 0, devices_all)
    counts = jnp.where(jnp.arange(devices_all) == busiest, CAP, counts)
    sub_keys = jax.random.split(key_perm, devices_all)

    def permute_one(subkey):
        return jax.random.permutation(subkey, tiles_dev)
    ranking = jax.vmap(permute_one)(sub_keys)
    significant = (ranking < counts[:, None]).astype(jnp.int32)
    return significant.reshape(blocks_r, blocks_c, A_DEV, B_DEV).transpose(0, 2, 1, 3).reshape(NA, NB)


def block_levels(rng, shape, shards, smallest, largest):
    def one(position, parts):
        steps = jax.random.uniform(jax.random.fold_in(jax.random.fold_in(rng, 6), position), (parts,), jnp.float32, smallest / len(shards), largest / len(shards))
        return jnp.repeat(jnp.exp(steps), shape[position] // parts).reshape((-1,) + (1,) * (len(shape) - position - 1))

    gain = one(*shards[0])
    for cut in shards[1:]:
        gain = gain * one(*cut)
    return gain


def noise(own_key, shape, scale, reach, cuts=(), kind=jnp.bfloat16):
    array = jax.random.normal(own_key, shape, jnp.float32) * scale
    if len(cuts) > 0:
        array = block_levels(own_key, shape, cuts, -0.22, 0.18) * array
    return jnp.clip(array, min=-reach, max=reach).astype(kind)


def setup_inputs(seed: int = 0) -> dict:
    arg_keys = jax.random.split(jax.random.key(seed), 5)
    return {
        "eri_tiles": noise(arg_keys[0], (NA, NB, PAIR, PAIR), (PAIR * (NA + NB) // 2) ** -0.5, 0.0625, ((0, 4), (1, 8))),
        "screen": draw_screen(jax.random.fold_in(arg_keys[4], 71), 0),
        "density_bra": noise(arg_keys[2], (NA * PAIR, DENS), 1.0, 6.0, ((0, 4), (1, 2))),
        "density_ket": noise(arg_keys[3], (NB * PAIR, DENS), 1.0, 6.0, ((0, 8), (1, 4))),
    }


def reference(eri_tiles, screen, density_bra, density_ket):
    keep = screen.astype(jnp.float32)
    ket_rows = density_ket.astype(jnp.float32).reshape(NB, PAIR, DENS)
    bra_rows = density_bra.astype(jnp.float32).reshape(NA, PAIR, DENS)

    def advance(carry, inputs):
        tiles, weights, bra_block = inputs
        masked = tiles.astype(jnp.float32) * weights[:, None, None]
        row_out = jnp.einsum('bij,bjr->ir', masked, ket_rows)
        carry = carry + jnp.einsum('bij,ir->bjr', masked, bra_block)
        return carry, row_out

    start_sum = jnp.zeros((NB, PAIR, DENS), jnp.float32)
    ket_total, bra_out = lax.scan(advance, start_sum, (eri_tiles, keep, bra_rows))
    return bra_out.reshape(NA * PAIR, DENS), ket_total.reshape(NB * PAIR, DENS)
```

```python
import functools

import jax
import jax.numpy as jnp
from jax import lax
from jax.experimental import pallas as pl
from jax.experimental.pallas import tpu as pltpu
from jax.sharding import PartitionSpec as P

MESH = pl.DeviceIdType.MESH
F32 = jnp.float32
KP = 2
SP = 4
BP = 2


def kernel(
    sizes, eri, screen, dbra, dket, out_b, out_k,
    scr, traw, tmat, kbuf, bbuf, kpart, k_rx, bp, d1_rx, x_rx, y_rx, fin,
    local_sem, ks_send, ks_recv, b_send, b_recv, kr_send, kr_recv,
    d1_send, d1_recv, x_send, x_recv, y_send, y_recv, f_send, f_recv,
):
    R, C, Dp = sizes
    per = R // C
    G = Dp // 2
    r, c, d = lax.axis_index("row"), lax.axis_index("col"), lax.axis_index("depth")
    h = d % 2
    g = d // 2
    sib = {"depth": d + 1 - 2 * h}
    A, B, PS = eri.shape[0], eri.shape[1], eri.shape[2]
    rows, cols = tmat.shape
    dk, kw = kbuf.shape[2], kbuf.shape[3]
    sw = kpart.shape[3]
    db = bbuf.shape[3]
    half = rows // 2
    bw = half // BP
    near = jnp.minimum(r, R - 1 - r)
    edge, inside = near == 0, near > 0
    pending = {"first": [], "last": []}

    def when(cond, fn):
        if cond is None:
            fn()
        else:
            pl.when(cond)(fn)

    def remote(src, dst, ssem, rsem, dev):
        return pltpu.make_async_remote_copy(
            src_ref=src, dst_ref=dst, send_sem=ssem, recv_sem=rsem, device_id=dev, device_id_type=MESH)

    def sent(cond, src, ssem, group="first"):
        pending[group].append((cond, lambda: remote(src, src, ssem, ssem, sib).wait_send()))

    def recv(dst, rsem):
        remote(dst, dst, rsem, rsem, sib).wait_recv()

    def flush(group):
        for cond, wait in pending[group]:
            when(cond, wait)

    loads = [
        pltpu.make_async_copy(dbra.at[pl.ds(0, half)], bbuf.at[c, 0], local_sem.at[0]),
        pltpu.make_async_copy(dbra.at[pl.ds(half, half)], bbuf.at[c, 1], local_sem.at[1]),
        pltpu.make_async_copy(eri, traw, local_sem.at[2]),
        pltpu.make_async_copy(screen, scr, local_sem.at[3 + KP]),
    ]
    kloads = [
        pltpu.make_async_copy(dket.at[:, pl.ds(u * kw, kw)], kbuf.at[r, u], local_sem.at[3 + u])
        for u in range(KP)
    ]
    for one in kloads:
        one.start()
    for one in loads:
        one.start()

    bar = pltpu.get_barrier_semaphore()

    def hello(dev):
        pl.semaphore_signal(bar, inc=1, device_id=dev, device_id_type=MESH)

    pl.when(r > 0)(lambda: hello({"row": r - 1}))
    pl.when(r < R - 1)(lambda: hello({"row": r + 1}))
    for o in range(1, C):
        hello({"col": (c + o) % C})
    hello(sib)
    for o in range(1, G):
        hello({"depth": (d + 2 * o) % Dp})
    pl.semaphore_wait(bar, C + G - 1 + jnp.where(r > 0, 1, 0) + jnp.where(r < R - 1, 1, 0))

    def ket_send(s, u, dirn, cond):
        pl.when(cond)(lambda: remote(
            kbuf.at[s, u], kbuf.at[s, u], ks_send.at[s, dirn], ks_recv.at[s, u], {"row": r - 1 + 2 * dirn}).start())

    for u in range(KP):
        kloads[u].wait()
        ket_send(r, u, 0, r > 0)
        ket_send(r, u, 1, r < R - 1)
    loads[0].wait()
    loads[1].wait()
    for o in range(1, C):
        remote(bbuf.at[c, h], bbuf.at[c, h], b_send.at[o], b_recv.at[0, c], {"col": (c + o) % C}).start()
        sent(None, bbuf.at[c, h], b_send.at[o])
    for dirn in range(2):
        sent((r < R - 1) if dirn else (r > 0), kbuf.at[r], ks_send.at[r, dirn])
    loads[2].wait()
    loads[3].wait()

    for a in range(A):
        for b in range(B):
            keep = scr[b, a] > 0
            tile = traw[a, b]
            tmat[a * PS:(a + 1) * PS, b * PS:(b + 1) * PS] = jnp.where(keep, tile, jnp.zeros_like(tile))

    def ket_block(cb):
        x = bbuf[cb].reshape(rows, db)
        res = lax.dot_general(x, tmat[...], (((0,), (0,)), ((), ())), preferred_element_type=F32)
        for j in range(per):
            for u in range(SP):
                kpart[cb * per + j, u] = res[j * dk:(j + 1) * dk, u * sw:(u + 1) * sw]

    def sum_send(t, u, dirn):
        remote(kpart.at[t, u], k_rx.at[dirn, t, u], kr_send.at[t], kr_recv.at[dirn, t, u],
               {"row": r - 1 + 2 * dirn}).start()

    mine = r // per == c

    def ket_ends(cb, which):
        for dirn in range(2):
            for j in range(per):
                t = cb * per + (per - 1 - j if dirn else j)
                go = (r == 0) & (t > r) if dirn else (r == R - 1) & (t < r)
                for u in range(SP):
                    ok = go
                    if which == "early" and u == SP - 1:
                        ok = go & jnp.logical_not(mine)
                    elif which == "rest":
                        if u < SP - 1:
                            continue
                        ok = go & mine
                    pl.when(ok)(functools.partial(sum_send, t, u, dirn))

    first = (c * 2) // C

    def flow(late, slot):
        dirn = 1 - first if late else first
        hop = jnp.where(dirn == 0, R - 1 - r, r)
        p = slot - 2 * (hop - 1) + (0 if late else 2)
        k, u = p // SP, p % SP
        t = jnp.where(dirn == 0, k, R - 1 - k)
        onward = R - 1 - hop

        def go():
            recv(k_rx.at[dirn, t, u], kr_recv.at[dirn, t, u])
            kpart[t, u] = kpart[t, u] + k_rx[dirn, t, u]
            pl.when(k < onward)(lambda: sum_send(t, u, dirn))
        pl.when((hop >= 1) & (p >= 0) & (k <= onward))(go)

    def slot_of(i):
        k = (i + 1) // 2
        inner = r - k if i % 2 == 1 else r + k
        inner = jnp.where(2 * r < R, 2 * r - inner, inner)
        outer = jnp.where(r > R - 1 - r, r - (i - near), r + (i - near))
        return jnp.where(i <= 2 * near, inner, outer)

    order = [slot_of(i) for i in range(R)]

    def ket_take(i, us, cond=None):
        s = order[i]

        def go():
            for u in us:
                recv(kbuf.at[s, u], ks_recv.at[s, u])
                ket_send(s, u, 0, (s > r) & (r > 0))
                ket_send(s, u, 1, (s < r) & (r < R - 1))
        when(cond, go)
        if us[-1] == KP - 1:
            def both(x):
                return x if cond is None else x & cond
            sent(both((s > r) & (r > 0)), kbuf.at[s], ks_send.at[s, 0])
            sent(both((s < r) & (r < R - 1)), kbuf.at[s], ks_send.at[s, 1])

    def bra_dot(i):
        s = order[i]
        res = sum(
            lax.dot_general(kbuf[s, u], tmat[:, u * kw:(u + 1) * kw], (((1,), (1,)), ((), ())),
                            preferred_element_type=F32)
            for u in range(KP))
        for q in range(BP):
            bp[s, 0, q] = res[:, q * bw:(q + 1) * bw]
            bp[s, 1, q] = res[:, half + q * bw:half + (q + 1) * bw]
        remote(bp.at[s, 1 - h], d1_rx.at[s], d1_send.at[s], d1_recv.at[s], sib).start()
        sent(None, bp.at[s, 1 - h], d1_send.at[s])

    def bra_b(i, cond=None):
        s = order[i]
        cs, j = s // per, s % per

        def go():
            recv(d1_rx.at[s], d1_recv.at[s])
            for q in range(BP):
                bp[s, h, q] = bp[s, h, q] + d1_rx[s, q]
                pl.when(cs != c)(lambda: remote(
                    bp.at[s, h, q], x_rx.at[c, j, q], x_send.at[s], x_recv.at[c, j, q], {"col": cs}).start())
        when(cond, go)
        sent(cs != c if cond is None else (cs != c) & cond, bp.at[s, h], x_send.at[s], "last")

    def bra_c(i, q, cond):
        s = order[i]
        cs, j = s // per, s % per

        def go():
            total = bp[s, h, q]
            for o in range(1, C):
                p = (c + o) % C
                recv(x_rx.at[p, j, q], x_recv.at[p, j, q])
                total = total + x_rx[p, j, q]
            y_rx[j, g, q] = total
            for o in range(1, G):
                remote(y_rx.at[j, g, q], y_rx.at[j, g, q], y_send.at[o, j], y_recv.at[j, g, q],
                       {"depth": (d + 2 * o) % Dp}).start()
        pl.when((cs == c) & cond)(go)

    def out_at(j, q, side):
        return pl.ds(pl.multiple_of(j * dk, 8), dk), pl.ds(pl.multiple_of(side * half + q * bw, 128), bw)

    def bra_d(i, q, cond):
        s = order[i]
        cs, j = s // per, s % per

        def go():
            for o in range(1, G):
                p = (g + o) % G
                recv(y_rx.at[j, p, q], y_recv.at[j, p, q])
            total = y_rx[j, 0, q]
            for p in range(1, G):
                total = total + y_rx[j, p, q]
            fin[j, q] = total
            at = out_at(j, q, h)
            remote(fin.at[j, q], out_b.at[at], f_send.at[j], f_recv.at[j, q], sib).start()
            out_b[at] = total
        pl.when((cs == c) & cond)(go)

    def bra_e():
        for j in range(per):
            for q in range(BP):
                recv(fin.at[j, q], f_recv.at[j, q])

    tail = []
    for late in (False, True):
        for slot in range(-2, (R - 1) * SP + 2 * R - 4):
            tail.append((10.5 + 1.4 * slot, functools.partial(flow, late, slot)))
    start_e = {0: 10.0, 1: 14.2, 2: 15.0, 3: 19.2}
    start_m = {0: 10.0, 2: 14.2, 1: 12.0, 3: 16.2}
    for i in range(R):
        for q in range(BP):
            for cond, table in ((edge, start_e), (inside, start_m)):
                at = table.get(i, 19.2 + 4.2 * (i - 3)) + 2.1 * q
                tail.append((at, functools.partial(bra_c, i, q, cond)))
                tail.append((at + 3.1, functools.partial(bra_d, i, q, cond)))
    tail.sort(key=lambda x: x[0])

    def run_tail(until):
        while tail and tail[0][0] < until:
            tail.pop(0)[1]()

    others = [(c + o) % C for o in range(1, C)]
    every = range(KP)
    ket_block(c)
    ket_ends(c, "early")
    bra_dot(0)
    ket_take(1, every, edge)
    for u in every:
        for i in (1, 2):
            ket_take(i, [u], inside)
    bra_dot(1)
    bra_b(0)
    for p in others:
        recv(bbuf.at[p, h], b_recv.at[0, p])
        remote(bbuf.at[p, h], bbuf.at[p, h], b_send.at[C + p], b_recv.at[1, p], sib).start()
        sent(None, bbuf.at[p, h], b_send.at[C + p])
    ket_take(3, [0], inside)
    bra_b(1)
    for p in others:
        recv(bbuf.at[p, 1 - h], b_recv.at[1, p])
        ket_block(p)
        ket_ends(p, "all")
    ket_ends(c, "rest")
    ket_take(3, list(range(1, KP)), inside)
    ket_take(2, every, edge)
    bra_dot(2)
    run_tail(10.0)
    ket_take(3, every, edge)
    bra_dot(3)
    bra_b(2)
    for i in range(4, R):
        ket_take(i, every)
        bra_dot(i)
        bra_b(i)
    run_tail(13.0)
    bra_b(3)
    run_tail(16.5)
    flush("first")
    run_tail(21.5)
    flush("last")
    pending["last"].clear()
    run_tail(1e9)
    bra_e()
    for u in range(SP):
        out_k[:, u * sw:(u + 1) * sw] = kpart[r, u]
    for t in range(R):
        sent(t != r, kpart.at[t], kr_send.at[t], "last")
    for j in range(per):
        for o in range(1, G):
            sent(None, y_rx.at[j, g], y_send.at[o, j], "last")
        sent(None, fin.at[j], f_send.at[j], "last")
    flush("last")


def body(sizes, eri_tiles, screen, density_bra, density_ket):
    R, C, Dp = sizes
    A, B, PS, _ = eri_tiles.shape
    rows, cols = A * PS, B * PS
    db, dk = density_bra.shape[1], density_ket.shape[1]
    per, G, half = R // C, Dp // 2, rows // 2
    DMA = pltpu.SemaphoreType.DMA
    hbm = pl.BlockSpec(memory_space=pltpu.HBM)
    vm = pl.BlockSpec(memory_space=pltpu.VMEM)
    piece = (dk, half // BP)
    out_b, out_k = pl.pallas_call(
        functools.partial(kernel, sizes),
        out_shape=(jax.ShapeDtypeStruct((db, rows), F32), jax.ShapeDtypeStruct((dk, cols), F32)),
        in_specs=[hbm, hbm, hbm, hbm],
        out_specs=(vm, vm),
        scratch_shapes=[
            pltpu.SMEM((B, A), jnp.int32),
            pltpu.VMEM((A, B, PS, PS), jnp.bfloat16),
            pltpu.VMEM((rows, cols), jnp.bfloat16),
            pltpu.VMEM((R, KP, dk, cols // KP), jnp.bfloat16),
            pltpu.VMEM((C, 2, half, db), jnp.bfloat16),
            pltpu.VMEM((R, SP, dk, cols // SP), F32),
            pltpu.VMEM((2, R, SP, dk, cols // SP), F32),
            pltpu.VMEM((R, 2, BP, *piece), F32),
            pltpu.VMEM((R, BP, *piece), F32),
            pltpu.VMEM((C, per, BP, *piece), F32),
            pltpu.VMEM((per, G, BP, *piece), F32),
            pltpu.VMEM((per, BP, *piece), F32),
            DMA((4 + KP,)),
            DMA((R, 2)), DMA((R, KP)),
            DMA((2 * C,)), DMA((2, C)),
            DMA((R,)), DMA((2, R, SP)),
            DMA((R,)), DMA((R,)),
            DMA((R,)), DMA((C, per, BP)),
            DMA((G, per)), DMA((per, G, BP)),
            DMA((per,)), DMA((per, BP)),
        ],
        compiler_params=pltpu.CompilerParams(
            collective_id=0, has_side_effects=True, vmem_limit_bytes=28 * 1024 * 1024),
    )(*(pltpu.with_memory_space_constraint(x, pltpu.HBM) for x in (eri_tiles, screen.T, density_bra, density_ket.T)))
    return out_b.T, out_k.T


def solution(mesh):
    sizes = (mesh.shape["row"], mesh.shape["col"], mesh.shape["depth"])
    return jax.shard_map(
        functools.partial(body, sizes),
        mesh=mesh,
        in_specs=(
            P("row", ("col", "depth"), None, None),
            P("row", ("col", "depth")),
            P("row", "col"),
            P(("col", "depth"), "row"),
        ),
        out_specs=(P("row", "col"), P(("col", "depth"), "row")),
        check_vma=False,
    )
```

```python
import functools

import jax
import jax.numpy as jnp
from jax import lax
from jax.experimental import pallas as pl
from jax.experimental.pallas import tpu as pltpu
from jax.sharding import PartitionSpec as P

MESH = pl.DeviceIdType.MESH
F32 = jnp.float32
KP = 2
SP = 4
HOPS = (5, 3)
BP = 3


def kernel(
    sizes, eri, screen, dbra, dket, out_b, out_k,
    scr, traw, tmat, kbuf, bbuf, kpart, k_rx, bp, d1_rx, x_rx, y_rx, fin,
    local_sem, send_sem, ks_recv, b_recv, kr_recv, d1_recv, x_recv, y_recv, f_recv,
):
    R, C, Dp = sizes
    per = R // C
    G = Dp // 2
    r, c, d = lax.axis_index("row"), lax.axis_index("col"), lax.axis_index("depth")
    h = d % 2
    g = d // 2
    sib = {"depth": d + 1 - 2 * h}
    A, B, PS = eri.shape[0], eri.shape[1], eri.shape[2]
    rows, cols = tmat.shape
    dk, kw = kbuf.shape[2], kbuf.shape[3]
    sw = kpart.shape[3]
    db = bbuf.shape[3]
    half = rows // 2
    bw = half // BP
    near = jnp.minimum(r, R - 1 - r)
    pending = {"first": [], "last": []}

    def when(cond, fn):
        if cond is None:
            fn()
        else:
            pl.when(cond)(fn)

    def remote(src, dst, rsem, dev):
        return pltpu.make_async_remote_copy(
            src_ref=src, dst_ref=dst, send_sem=send_sem, recv_sem=rsem, device_id=dev, device_id_type=MESH)

    def sent(cond, src, group="first"):
        pending[group].append((cond, lambda: remote(src, src, send_sem, sib).wait_send()))

    def recv(dst, rsem):
        remote(dst, dst, rsem, sib).wait_recv()

    def flush(group):
        for cond, wait in pending[group]:
            when(cond, wait)

    loads = [
        pltpu.make_async_copy(dbra.at[pl.ds(0, half)], bbuf.at[c, 0], local_sem.at[0]),
        pltpu.make_async_copy(dbra.at[pl.ds(half, half)], bbuf.at[c, 1], local_sem.at[1]),
        pltpu.make_async_copy(eri, traw, local_sem.at[2]),
        pltpu.make_async_copy(screen, scr, local_sem.at[3 + KP]),
    ]
    kloads = [
        pltpu.make_async_copy(dket.at[:, pl.ds(u * kw, kw)], kbuf.at[r, u], local_sem.at[3 + u])
        for u in range(KP)
    ]
    for one in kloads:
        one.start()
    for one in loads:
        one.start()

    bar = pltpu.get_barrier_semaphore()

    def hello(dev):
        pl.semaphore_signal(bar, inc=1, device_id=dev, device_id_type=MESH)

    pl.when(r > 0)(lambda: hello({"row": r - 1}))
    pl.when(r < R - 1)(lambda: hello({"row": r + 1}))
    for o in range(1, C):
        hello({"col": (c + o) % C})
    hello(sib)
    for o in range(1, G):
        hello({"depth": (d + 2 * o) % Dp})
    pl.semaphore_wait(bar, C + G - 1 + jnp.where(r > 0, 1, 0) + jnp.where(r < R - 1, 1, 0))

    def ket_send(s, u, dirn, cond):
        pl.when(cond)(lambda: remote(
            kbuf.at[s, u], kbuf.at[s, u], ks_recv.at[s, u], {"row": r - 1 + 2 * dirn}).start())

    for u in range(KP):
        kloads[u].wait()
        ket_send(r, u, 0, r > 0)
        ket_send(r, u, 1, r < R - 1)
    loads[0].wait()
    loads[1].wait()
    for o in range(1, C):
        remote(bbuf.at[c, h], bbuf.at[c, h], b_recv.at[0, C - 1 - o], {"col": (c + o) % C}).start()
        sent(None, bbuf.at[c, h])
    for dirn in range(2):
        sent((r < R - 1) if dirn else (r > 0), kbuf.at[r])
    loads[2].wait()
    loads[3].wait()

    for a in range(A):
        for b in range(B):
            keep = scr[b, a] > 0
            tile = traw[a, b]
            tmat[a * PS:(a + 1) * PS, b * PS:(b + 1) * PS] = jnp.where(keep, tile, jnp.zeros_like(tile))

    def ket_block(cb):
        x = bbuf[cb].reshape(rows, db)
        res = lax.dot_general(x, tmat[...], (((0,), (0,)), ((), ())), preferred_element_type=F32)
        for j in range(per):
            for u in range(SP):
                kpart[cb * per + j, u] = res[j * dk:(j + 1) * dk, u * sw:(u + 1) * sw]

    def sum_send(t, u, dirn):
        remote(kpart.at[t, u], k_rx.at[dirn, t, u], kr_recv.at[t + dirn, u],
               {"row": r - 1 + 2 * dirn}).start()

    mine = r // per == c

    def ket_ends(cb, pieces, only=None):
        for dirn in range(2):
            for j in range(per):
                t = cb * per + (per - 1 - j if dirn else j)
                go = (r == 0) & (t > r) if dirn else (r == R - 1) & (t < r)
                for u in pieces:
                    ok = go if only is None or u < SP - 1 and not only else go & (mine if only else ~mine)
                    pl.when(ok)(functools.partial(sum_send, t, u, dirn))

    first = (c * 2) // C

    def flow(late, p):
        dirn = 1 - first if late else first
        hop = jnp.where(dirn == 0, R - 1 - r, r)

        def go(p):
            k, u = p // SP, p % SP
            t = jnp.where(dirn == 0, k, R - 1 - k)
            recv(k_rx.at[dirn, t, u], kr_recv.at[t + dirn, u])
            kpart[t, u] = kpart[t, u] + k_rx[dirn, t, u]
            pl.when(k < R - 1 - hop)(lambda: sum_send(t, u, dirn))
        p = p - HOPS[late] * (hop - 1)
        pl.when((hop >= 1) & (p >= 0) & (p < (R - hop) * SP))(lambda: go(p))

    def slot_of(i):
        k = (i + 1) // 2
        inner = r - k if i % 2 == 1 else r + k
        inner = jnp.where(2 * r < R, 2 * r - inner, inner)
        outer = jnp.where(r > R - 1 - r, r - (i - near), r + (i - near))
        return jnp.where(i <= 2 * near, inner, outer)

    order = [slot_of(i) for i in range(R)]

    def ket_take(i, u):
        s = order[i]
        recv(kbuf.at[s, u], ks_recv.at[s, u])
        for dirn, on in ((0, (s > r) & (r > 0)), (1, (s < r) & (r < R - 1))):
            ket_send(s, u, dirn, on)
            if u == KP - 1:
                sent(on, kbuf.at[s])

    def bra_dot(i, u):
        s = order[i]
        for side, other in ((1 - h, True), (h, False)):
            part = tmat[pl.ds(pl.multiple_of(side * half, 128), half), u * kw:(u + 1) * kw]
            res = lax.dot_general(kbuf[s, u], part, (((1,), (1,)), ((), ())), preferred_element_type=F32)
            for q in range(BP):
                term = res[:, q * bw:(q + 1) * bw]
                bp[s, side, q] = term if u == 0 else bp[s, side, q] + term
            if other and u == KP - 1:
                for q in range(BP):
                    remote(bp.at[s, side, q], d1_rx.at[s, q], d1_recv.at[s, q], sib).start()
        if u == KP - 1:
            sent(None, bp.at[s, 1 - h])

    def bra_b(i):
        s = order[i]
        cs, j = s // per, s % per
        for q in range(BP):
            recv(d1_rx.at[s, q], d1_recv.at[s, q])
            bp[s, h, q] = bp[s, h, q] + d1_rx[s, q]
            pl.when(cs != c)(lambda: remote(
                bp.at[s, h, q], x_rx.at[c, j, q], x_recv.at[(c - cs + C - 1) % C, j, q], {"col": cs}).start())
        sent(cs != c, bp.at[s, h], "last")

    def bra_c(i, q):
        s = order[i]
        cs, j = s // per, s % per

        def go():
            total = bp[s, h, q]
            for o in range(1, C):
                p = (c + o) % C
                recv(x_rx.at[p, j, q], x_recv.at[o - 1, j, q])
                total = total + x_rx[p, j, q]
            y_rx[j, g, q] = total
            for o in range(1, G):
                remote(y_rx.at[j, g, q], y_rx.at[j, g, q], y_recv.at[j, G - 1 - o, q],
                       {"depth": (d + 2 * o) % Dp}).start()
        pl.when(cs == c)(go)

    def out_at(j, q, side):
        return pl.ds(pl.multiple_of(j * dk, 8), dk), pl.ds(pl.multiple_of(side * half + q * bw, 128), bw)

    def bra_d(i, q):
        s = order[i]
        cs, j = s // per, s % per

        def go():
            for o in range(1, G):
                p = (g + o) % G
                recv(y_rx.at[j, p, q], y_recv.at[j, o - 1, q])
            total = y_rx[j, 0, q]
            for p in range(1, G):
                total = total + y_rx[j, p, q]
            fin[j, q] = total
            at = out_at(j, q, h)
            remote(fin.at[j, q], out_b.at[at], f_recv, sib).start()
            out_b[at] = total
        pl.when(cs == c)(go)

    def bra_e():
        recv(fin, f_recv)

    others = [(c + o) % C for o in range(1, C)]

    def bra_forward():
        for o, p in enumerate(others):
            recv(bbuf.at[p, h], b_recv.at[0, o])
            remote(bbuf.at[p, h], bbuf.at[p, h], b_recv.at[1, o], sib).start()
            sent(None, bbuf.at[p, h])

    def ket_others():
        for o, p in enumerate(others):
            recv(bbuf.at[p, 1 - h], b_recv.at[1, o])
            ket_block(p)
            ket_ends(p, range(SP))

    def start_edge():
        ket_ends(c, range(SP), False)
        for u in range(KP):
            bra_dot(0, u)
        for u in range(KP):
            ket_take(1, u)
            bra_dot(1, u)
        bra_forward()
        bra_b(0)
        ket_others()
        ket_ends(c, [SP - 1], True)
        bra_b(1)
        for u in range(KP):
            ket_take(2, u)
            bra_dot(2, u)
        for i in range(3, R):
            bra_b(i - 1)
            for u in range(KP):
                ket_take(i, u)
                bra_dot(i, u)
        return R - 1

    def start_inside():
        for u in range(KP):
            bra_dot(0, u)
        for u in range(KP):
            ket_take(1, u)
            ket_take(2, u)
            bra_dot(1, u)
        bra_b(0)
        for u in range(KP):
            bra_dot(2, u)
        bra_forward()
        for u in range(KP):
            ket_take(3, u)
            bra_dot(3, u)
            if u == 0:
                bra_b(1)
        ket_others()
        bra_b(2)
        for i in range(4, R):
            for u in range(KP):
                ket_take(i, u)
                bra_dot(i, u)
            bra_b(i - 1)
        return R - 1

    def finish(kind, last):
        tail = [(16.1 if kind == "edge" else 12.1, bra_b, (last,))]
        for late in (False, True):
            lag = HOPS[late]
            if kind == "edge":
                steps = range(lag * (R - 2), lag * (R - 2) + SP)
            else:
                steps = range(max((R - hop) * SP + lag * (hop - 1) for hop in range(1, R - 1)))
            for p in steps:
                tail.append(((13.0 if late else 8.9) + 1.4 * p, flow, (late, p)))
        start = {0: 11.3, 1: 15.5, 2: 16.1, 3: 20.3} if kind == "edge" else {0: 11.2, 2: 15.2, 1: 13.4, 3: 17.6}
        for i in range(R):
            for q in range(BP):
                at = start.get(i, 20.3 + 4.2 * (i - 3)) + 4.2 / BP * q
                tail.append((at, bra_c, (i, q)))
                tail.append((at + 2.2 + 4.2 / BP, bra_d, (i, q)))
        tail.sort(key=lambda x: x[0])
        first_done = last_done = False
        for at, fn, args in tail:
            if at > 19 and not first_done:
                flush("first")
                first_done = True
            if at > 23.6 and not last_done:
                flush("last")
                last_done = True
            fn(*args)
        bra_e()
        for u in range(SP):
            out_k[:, u * sw:(u + 1) * sw] = kpart[r, u]
        pending["last"].clear()
        for t in range(R):
            sent(t != r, kpart.at[t], "last")
        for j in range(per):
            for o in range(1, G):
                sent(None, y_rx.at[j, g], "last")
            sent(None, fin.at[j], "last")
        flush("last")

    ket_block(c)
    front = list(pending["first"])

    def run(kind):
        pending["first"], pending["last"] = list(front), []
        finish(kind, start_edge() if kind == "edge" else start_inside())

    pl.when(near == 0)(lambda: run("edge"))
    pl.when(near > 0)(lambda: run("inside"))


def body(sizes, eri_tiles, screen, density_bra, density_ket):
    R, C, Dp = sizes
    A, B, PS, _ = eri_tiles.shape
    rows, cols = A * PS, B * PS
    db, dk = density_bra.shape[1], density_ket.shape[1]
    per, G, half = R // C, Dp // 2, rows // 2
    DMA = pltpu.SemaphoreType.DMA
    hbm = pl.BlockSpec(memory_space=pltpu.HBM)
    vm = pl.BlockSpec(memory_space=pltpu.VMEM)
    piece = (dk, half // BP)
    out_b, out_k = pl.pallas_call(
        functools.partial(kernel, sizes),
        out_shape=(jax.ShapeDtypeStruct((db, rows), F32), jax.ShapeDtypeStruct((dk, cols), F32)),
        in_specs=[hbm, hbm, hbm, hbm],
        out_specs=(vm, vm),
        scratch_shapes=[
            pltpu.SMEM((B, A), jnp.int32),
            pltpu.VMEM((A, B, PS, PS), jnp.bfloat16),
            pltpu.VMEM((rows, cols), jnp.bfloat16),
            pltpu.VMEM((R, KP, dk, cols // KP), jnp.bfloat16),
            pltpu.VMEM((C, 2, half, db), jnp.bfloat16),
            pltpu.VMEM((R, SP, dk, cols // SP), F32),
            pltpu.VMEM((2, R, SP, dk, cols // SP), F32),
            pltpu.VMEM((R, 2, BP, *piece), F32),
            pltpu.VMEM((R, BP, *piece), F32),
            pltpu.VMEM((C, per, BP, *piece), F32),
            pltpu.VMEM((per, G, BP, *piece), F32),
            pltpu.VMEM((per, BP, *piece), F32),
            DMA((4 + KP,)), DMA, DMA((R, KP)), DMA((2, C - 1)), DMA((R + 1, SP)),
            DMA((R, BP)), DMA((C - 1, per, BP)), DMA((per, G - 1, BP)), DMA,
        ],
        compiler_params=pltpu.CompilerParams(
            collective_id=0, has_side_effects=True, vmem_limit_bytes=28 * 1024 * 1024),
    )(*(pltpu.with_memory_space_constraint(x, pltpu.HBM) for x in (eri_tiles, screen.T, density_bra, density_ket.T)))
    return out_b.T, out_k.T


def solution(mesh):
    sizes = (mesh.shape["row"], mesh.shape["col"], mesh.shape["depth"])
    return jax.shard_map(
        functools.partial(body, sizes),
        mesh=mesh,
        in_specs=(
            P("row", ("col", "depth"), None, None),
            P("row", ("col", "depth")),
            P("row", "col"),
            P(("col", "depth"), "row"),
        ),
        out_specs=(P("row", "col"), P(("col", "depth"), "row")),
        check_vma=False,
    )
```

```python
import functools

import jax
import jax.numpy as jnp
from jax import lax
from jax.experimental import pallas as pl
from jax.experimental.pallas import tpu as pltpu
from jax.sharding import PartitionSpec as P

MESH = pl.DeviceIdType.MESH
F32 = jnp.float32
BF16 = jnp.bfloat16
STEPS = 7 * 2.0**8
KP = 4
KD = 2
SP = 4
HOPS = (8, 4)
STORES = 4
BP = 3


def pack(ref, v):
    w = v.shape[1]
    top = v.astype(BF16)
    near = top.astype(F32)
    rest = jnp.round((v - near) / jnp.where(near == 0, 1.0, near) * STEPS)
    ref[:, :w] = top
    ref[:, w:] = (rest[:, :w // 2] * 16 + rest[:, w // 2:]).astype(BF16)


def unpack(ref):
    w = ref.shape[1] * 2 // 3
    near = ref[:, :w].astype(F32)
    both = ref[:, w:].astype(F32)
    high = jnp.round(both * (1 / 16))
    rest = jnp.concatenate([high, both - high * 16], 1)
    return near + near * rest * (1 / STEPS)


def kernel(
    sizes, eri, screen, dbra, dket, out_b, out_k,
    scr, traw, tmat, kbuf, bbuf, kpart, k_tx, k_rx, bp, d1_rx, x_tx, x_rx, y_rx, fin,
    local_sem, send_sem, ks_recv, b_recv, kr_recv, d1_recv, x_recv, y_recv, f_recv,
):
    R, C, Dp = sizes
    per = R // C
    G = Dp // 2
    r, c, d = lax.axis_index("row"), lax.axis_index("col"), lax.axis_index("depth")
    h = d % 2
    g = d // 2
    sib = {"depth": d + 1 - 2 * h}
    A, B, PS = eri.shape[0], eri.shape[1], eri.shape[2]
    rows, cols = A * PS, B * PS
    dk, kw = kbuf.shape[2], kbuf.shape[3]
    sw = kpart.shape[3]
    db = bbuf.shape[3]
    half = rows // 2
    bw = half // BP
    near = jnp.minimum(r, R - 1 - r)
    pending = {"first": [], "last": []}

    def when(cond, fn):
        if cond is None:
            fn()
        else:
            pl.when(cond)(fn)

    def remote(src, dst, rsem, dev):
        return pltpu.make_async_remote_copy(
            src_ref=src, dst_ref=dst, send_sem=send_sem, recv_sem=rsem, device_id=dev, device_id_type=MESH)

    def sent(cond, src, group="first"):
        pending[group].append((cond, lambda: remote(src, src, send_sem, sib).wait_send()))

    def recv(dst, rsem):
        remote(dst, dst, rsem, sib).wait_recv()

    def flush(group):
        for cond, wait in pending[group]:
            when(cond, wait)

    loads = [
        pltpu.make_async_copy(dbra.at[pl.ds(0, half)], bbuf.at[c, 0], local_sem.at[0]),
        pltpu.make_async_copy(dbra.at[pl.ds(half, half)], bbuf.at[c, 1], local_sem.at[1]),
        pltpu.make_async_copy(eri, traw, local_sem.at[2]),
        pltpu.make_async_copy(screen, scr, local_sem.at[3 + KP]),
    ]
    kloads = [
        pltpu.make_async_copy(dket.at[:, pl.ds(u * kw, kw)], kbuf.at[r, u], local_sem.at[3 + u])
        for u in range(KP)
    ]
    for one in kloads:
        one.start()
    for one in loads:
        one.start()

    bar = pltpu.get_barrier_semaphore()

    def hello(dev):
        pl.semaphore_signal(bar, inc=1, device_id=dev, device_id_type=MESH)

    pl.when(r > 0)(lambda: hello({"row": r - 1}))
    pl.when(r < R - 1)(lambda: hello({"row": r + 1}))
    for o in range(1, C):
        hello({"col": (c + o) % C})
    hello(sib)
    for o in range(1, G):
        hello({"depth": (d + 2 * o) % Dp})
    pl.semaphore_wait(bar, C + G - 1 + jnp.where(r > 0, 1, 0) + jnp.where(r < R - 1, 1, 0))

    def ket_send(s, u, dirn, cond):
        pl.when(cond)(lambda: remote(
            kbuf.at[s, u], kbuf.at[s, u], ks_recv.at[s, u], {"row": r - 1 + 2 * dirn}).start())

    for u in range(KP):
        kloads[u].wait()
        ket_send(r, u, 0, r > 0)
        ket_send(r, u, 1, r < R - 1)
    loads[0].wait()
    loads[1].wait()
    for o in range(1, C):
        remote(bbuf.at[c, h], bbuf.at[c, h], b_recv.at[0, C - 1 - o], {"col": (c + o) % C}).start()
        sent(None, bbuf.at[c, h])
    for dirn in range(2):
        sent((r < R - 1) if dirn else (r > 0), kbuf.at[r])
    loads[2].wait()
    loads[3].wait()

    for a in range(A):
        for b in range(B):
            keep = scr[b, a] > 0
            tile = traw[a, b]
            at = a % (A // 2) * PS
            tmat[a // (A // 2), at:at + PS, b * PS:(b + 1) * PS] = jnp.where(keep, tile, jnp.zeros_like(tile))

    def ket_block(cb):
        x = bbuf[cb].reshape(rows, db)
        res = lax.dot_general(x, tmat[...].reshape(rows, cols), (((0,), (0,)), ((), ())), preferred_element_type=F32)
        for j in range(per):
            for u in range(SP):
                kpart[cb * per + j, u] = res[j * dk:(j + 1) * dk, u * sw:(u + 1) * sw]

    def sum_send(t, u, dirn):
        pack(k_tx.at[t, u], kpart[t, u])
        remote(k_tx.at[t, u], k_rx.at[dirn, t, u], kr_recv.at[t + dirn, u], {"row": r - 1 + 2 * dirn}).start()

    mine = r // per == c

    def ket_ends(cb, pieces, only=None):
        for dirn in range(2):
            for j in range(per):
                t = cb * per + (per - 1 - j if dirn else j)
                go = (r == 0) & (t > r) if dirn else (r == R - 1) & (t < r)
                for u in pieces:
                    ok = go if only is None or u < SP - 1 and not only else go & (mine if only else ~mine)
                    pl.when(ok)(functools.partial(sum_send, t, u, dirn))

    first = (c * 2) // C

    def flow(late, p):
        dirn = 1 - first if late else first
        hop = jnp.where(dirn == 0, R - 1 - r, r)

        def go(p):
            k, u = p // SP, p % SP
            t = jnp.where(dirn == 0, k, R - 1 - k)
            recv(k_rx.at[dirn, t, u], kr_recv.at[t + dirn, u])
            kpart[t, u] = kpart[t, u] + unpack(k_rx.at[dirn, t, u])
            pl.when(k < R - 1 - hop)(lambda: sum_send(t, u, dirn))
        p = p - HOPS[late] * (hop - 1)
        pl.when((hop >= 1) & (p >= 0) & (p < (R - hop) * SP))(lambda: go(p))

    def slot_of(i):
        k = (i + 1) // 2
        inner = r - k if i % 2 == 1 else r + k
        inner = jnp.where(2 * r < R, 2 * r - inner, inner)
        outer = jnp.where(r > R - 1 - r, r - (i - near), r + (i - near))
        return jnp.where(i <= 2 * near, inner, outer)

    order = [slot_of(i) for i in range(R)]

    def ket_take(i, u):
        s = order[i]
        recv(kbuf.at[s, u], ks_recv.at[s, u])
        for dirn, on in ((0, (s > r) & (r > 0)), (1, (s < r) & (r < R - 1))):
            ket_send(s, u, dirn, on)
            if u == KP - 1:
                sent(on, kbuf.at[s])

    def bra_dot(i, u):
        s = order[i]
        for side, other in ((1 - h, True), (h, False)):
            part = tmat[side, :, u * kw * KP // KD:(u + 1) * kw * KP // KD]
            left = jnp.concatenate([kbuf[s, u * KP // KD + v] for v in range(KP // KD)], 1)
            res = lax.dot_general(left, part, (((1,), (1,)), ((), ())), preferred_element_type=F32)
            for q in range(BP):
                term = res[:, q * bw:(q + 1) * bw]
                bp[s, side, q] = term if u == 0 else bp[s, side, q] + term
            if other and u == KD - 1:
                for q in range(BP):
                    remote(bp.at[s, side, q], d1_rx.at[s, q], d1_recv.at[s, q], sib).start()
        if u == KD - 1:
            sent(None, bp.at[s, 1 - h])

    def bra_b(i):
        s = order[i]
        cs, j = s // per, s % per
        for q in range(BP):
            recv(d1_rx.at[s, q], d1_recv.at[s, q])
            total = bp[s, h, q] + d1_rx[s, q]
            bp[s, h, q] = total

            def go():
                pack(x_tx.at[s, q], total)
                remote(x_tx.at[s, q], x_rx.at[c, j, q], x_recv.at[(c - cs + C - 1) % C, j, q], {"col": cs}).start()
            pl.when(cs != c)(go)
        sent(cs != c, x_tx.at[s], "last")

    def bra_c(i, q):
        s = order[i]
        cs, j = s // per, s % per

        def go():
            total = bp[s, h, q]
            for o in range(1, C):
                p = (c + o) % C
                recv(x_rx.at[p, j, q], x_recv.at[o - 1, j, q])
                total = total + unpack(x_rx.at[p, j, q])
            pack(y_rx.at[j, g, q], total)
            for o in range(1, G):
                remote(y_rx.at[j, g, q], y_rx.at[j, g, q], y_recv.at[j, G - 1 - o, q],
                       {"depth": (d + 2 * o) % Dp}).start()
        pl.when(cs == c)(go)

    def out_at(j, q, side):
        return pl.ds(pl.multiple_of(j * dk, 8), dk), pl.ds(pl.multiple_of(side * half + q * bw, 128), bw)

    def bra_d(i, q):
        s = order[i]
        cs, j = s // per, s % per

        def go():
            for o in range(1, G):
                p = (g + o) % G
                recv(y_rx.at[j, p, q], y_recv.at[j, o - 1, q])
            total = unpack(y_rx.at[j, 0, q])
            for p in range(1, G):
                total = total + unpack(y_rx.at[j, p, q])
            fin[j, q] = total
            at = out_at(j, q, h)
            remote(fin.at[j, q], out_b.at[at], f_recv, sib).start()
            out_b[at] = total
        pl.when(cs == c)(go)

    def bra_e():
        recv(fin, f_recv)

    others = [(c + o) % C for o in range(1, C)]

    def bra_forward():
        for o, p in enumerate(others):
            recv(bbuf.at[p, h], b_recv.at[0, o])
            remote(bbuf.at[p, h], bbuf.at[p, h], b_recv.at[1, o], sib).start()
            sent(None, bbuf.at[p, h])

    def ket_others():
        for o, p in enumerate(others):
            recv(bbuf.at[p, 1 - h], b_recv.at[1, o])
            ket_block(p)
            ket_ends(p, range(SP))

    def take_dot(i, u, *more):
        for v in range(KP // KD):
            for k in (i, *more):
                ket_take(k, u * KP // KD + v)
        bra_dot(i, u)

    def start_edge():
        ket_ends(c, range(SP), False)
        for u in range(KD):
            bra_dot(0, u)
        for u in range(KD):
            take_dot(1, u)
        bra_forward()
        bra_b(0)
        ket_others()
        ket_ends(c, [SP - 1], True)
        bra_b(1)
        for u in range(KD):
            take_dot(2, u)
        for i in range(3, R):
            bra_b(i - 1)
            for u in range(KD):
                take_dot(i, u)
        return R - 1

    def start_inside():
        for u in range(KD):
            bra_dot(0, u)
        for u in range(KD):
            take_dot(1, u, 2)
        bra_b(0)
        for u in range(KD):
            bra_dot(2, u)
        bra_forward()
        for u in range(KD):
            take_dot(3, u)
            if u == 0:
                bra_b(1)
        ket_others()
        bra_b(2)
        for i in range(4, R):
            for u in range(KD):
                take_dot(i, u)
            bra_b(i - 1)
        return R - 1

    def finish(kind, last):
        tail = [(10.0 if kind == "edge" else 12.1, bra_b, (last,))]
        for late in (False, True):
            lag = HOPS[late]
            if kind == "edge":
                steps = range(lag * (R - 2), lag * (R - 2) + SP)
            else:
                steps = range(max((R - hop) * SP + lag * (hop - 1) for hop in range(1, R - 1)))
            for p in steps:
                tail.append(((13.5 if late else 8.5) + 1.05 * p, flow, (late, p)))
        start = {0: 11.3, 1: 14.5, 2: 15.6, 3: 20.0} if kind == "edge" else {0: 11.2, 2: 16.0, 1: 13.4, 3: 16.6}
        for i in range(R):
            for q in range(BP):
                at = start.get(i, 20.0 + 4.2 * (i - 3)) + 3.2 / BP * q
                tail.append((at, bra_c, (i, q)))
                tail.append((at + 2.5 + 3.2 / BP, bra_d, (i, q)))
        tail.sort(key=lambda x: x[0])
        first_done = last_done = False
        for at, fn, args in tail:
            if at > 19 and not first_done:
                flush("first")
                first_done = True
            if at > 23.6 and not last_done:
                flush("last")
                last_done = True
            fn(*args)
        bra_e()
        for u in range(SP):
            out_k[:, u * sw:(u + 1) * sw] = kpart[r, u]
        pending["last"].clear()
        for t in range(R):
            sent(t != r, k_tx.at[t], "last")
        for j in range(per):
            for o in range(1, G):
                sent(None, y_rx.at[j, g], "last")
            sent(None, fin.at[j], "last")
        flush("last")

    ket_block(c)
    front = list(pending["first"])

    def run(kind):
        pending["first"], pending["last"] = list(front), []
        finish(kind, start_edge() if kind == "edge" else start_inside())

    pl.when(near == 0)(lambda: run("edge"))
    pl.when(near > 0)(lambda: run("inside"))


def store(bra_t, ket_t, bra, ket, turned, sem):
    kets = pltpu.make_async_copy(ket_t, ket, sem.at[0])
    kets.start()
    size = turned.shape[0] // STORES
    copies = []
    for i in range(STORES):
        at = pl.ds(i * size, size)
        turned[at] = bra_t[:, at].T
        copies.append(pltpu.make_async_copy(turned.at[at], bra.at[at], sem.at[1 + i]))
        copies[-1].start()
    for one in [kets, *copies]:
        one.wait()


def body(sizes, eri_tiles, screen, density_bra, density_ket):
    R, C, Dp = sizes
    A, B, PS, _ = eri_tiles.shape
    rows, cols = A * PS, B * PS
    db, dk = density_bra.shape[1], density_ket.shape[1]
    per, G, half = R // C, Dp // 2, rows // 2
    DMA = pltpu.SemaphoreType.DMA
    hbm = pl.BlockSpec(memory_space=pltpu.HBM)
    vm = pl.BlockSpec(memory_space=pltpu.VMEM)
    piece, coded = (dk, half // BP), (dk, half // BP * 3 // 2)
    out_b, out_k = pl.pallas_call(
        functools.partial(kernel, sizes),
        out_shape=(jax.ShapeDtypeStruct((db, rows), F32), jax.ShapeDtypeStruct((dk, cols), F32)),
        in_specs=[hbm, hbm, hbm, hbm],
        out_specs=(vm, vm),
        scratch_shapes=[
            pltpu.SMEM((B, A), jnp.int32),
            pltpu.VMEM((A, B, PS, PS), BF16),
            pltpu.VMEM((2, half, cols), BF16),
            pltpu.VMEM((R, KP, dk, cols // KP), BF16),
            pltpu.VMEM((C, 2, half, db), BF16),
            pltpu.VMEM((R, SP, dk, cols // SP), F32),
            pltpu.VMEM((R, SP, dk, cols // SP * 3 // 2), BF16),
            pltpu.VMEM((2, R, SP, dk, cols // SP * 3 // 2), BF16),
            pltpu.VMEM((R, 2, BP, *piece), F32),
            pltpu.VMEM((R, BP, *piece), F32),
            pltpu.VMEM((R, BP, *coded), BF16),
            pltpu.VMEM((C, per, BP, *coded), BF16),
            pltpu.VMEM((per, G, BP, *coded), BF16),
            pltpu.VMEM((per, BP, *piece), F32),
            DMA((4 + KP,)), DMA, DMA((R, KP)), DMA((2, C - 1)), DMA((R + 1, SP)),
            DMA((R, BP)), DMA((C - 1, per, BP)), DMA((per, G - 1, BP)), DMA,
        ],
        compiler_params=pltpu.CompilerParams(
            collective_id=0, has_side_effects=True, vmem_limit_bytes=28 * 1024 * 1024),
    )(*(pltpu.with_memory_space_constraint(x, pltpu.HBM) for x in (eri_tiles, screen.T, density_bra, density_ket.T)))
    bra, ket = pl.pallas_call(
        store,
        out_shape=(jax.ShapeDtypeStruct((rows, db), F32), jax.ShapeDtypeStruct((dk, cols), F32)),
        in_specs=[vm, vm],
        out_specs=(hbm, hbm),
        scratch_shapes=[pltpu.VMEM((rows, db), F32), DMA((1 + STORES,))],
        compiler_params=pltpu.CompilerParams(vmem_limit_bytes=4 * 1024 * 1024),
    )(out_b, out_k)
    return bra, ket.T


def solution(mesh):
    sizes = (mesh.shape["row"], mesh.shape["col"], mesh.shape["depth"])
    return jax.shard_map(
        functools.partial(body, sizes),
        mesh=mesh,
        in_specs=(
            P("row", ("col", "depth"), None, None),
            P("row", ("col", "depth")),
            P("row", "col"),
            P(("col", "depth"), "row"),
        ),
        out_specs=(P("row", "col"), P(("col", "depth"), "row")),
        check_vma=False,
    )
```

```python
import functools

import jax
import jax.numpy as jnp
from jax import lax
from jax.experimental import pallas as pl
from jax.experimental.pallas import tpu as pltpu
from jax.sharding import PartitionSpec as P

MESH = pl.DeviceIdType.MESH
F32 = jnp.float32
BF16 = jnp.bfloat16
STEPS = 7 * 2.0**8
KP = 4
SP = 4
HOPS = (6, 4)
STORES = 4
BP = 3


def pack(ref, v):
    w = v.shape[1]
    top = v.astype(BF16)
    near = top.astype(F32)
    rest = jnp.round((v - near) / jnp.where(near == 0, 1.0, near) * STEPS)
    ref[:, :w] = top
    ref[:, w:] = (rest[:, :w // 2] * 16 + rest[:, w // 2:]).astype(BF16)


def unpack(ref):
    w = ref.shape[1] * 2 // 3
    near = ref[:, :w].astype(F32)
    both = ref[:, w:].astype(F32)
    high = jnp.round(both * (1 / 16))
    rest = jnp.concatenate([high, both - high * 16], 1)
    return near + near * rest * (1 / STEPS)


def kernel(
    sizes, eri, screen, dbra, dket, out_b, out_k,
    scr, traw, tmat, kbuf, bbuf, kpart, k_tx, k_rx, bp, d1_rx, x_tx, x_rx, y_rx, fin,
    local_sem, send_sem, ks_recv, b_recv, kr_recv, d1_recv, x_recv, y_recv, f_recv,
):
    R, C, Dp = sizes
    per = R // C
    G = Dp // 2
    r, c, d = lax.axis_index("row"), lax.axis_index("col"), lax.axis_index("depth")
    h = d % 2
    g = d // 2
    sib = {"depth": d + 1 - 2 * h}
    A, B, PS = eri.shape[0], eri.shape[1], eri.shape[2]
    rows, cols = A * PS, B * PS
    dk, kw = kbuf.shape[2], kbuf.shape[3]
    sw = kpart.shape[3]
    db = bbuf.shape[3]
    half = rows // 2
    bw = half // BP
    near = jnp.minimum(r, R - 1 - r)
    pending = {"first": [], "last": []}

    def when(cond, fn):
        if cond is None:
            fn()
        else:
            pl.when(cond)(fn)

    def remote(src, dst, rsem, dev):
        return pltpu.make_async_remote_copy(
            src_ref=src, dst_ref=dst, send_sem=send_sem, recv_sem=rsem, device_id=dev, device_id_type=MESH)

    def sent(cond, src, group="first"):
        pending[group].append((cond, lambda: remote(src, src, send_sem, sib).wait_send()))

    def recv(dst, rsem):
        remote(dst, dst, rsem, sib).wait_recv()

    def flush(group):
        for cond, wait in pending[group]:
            when(cond, wait)

    loads = [
        pltpu.make_async_copy(dbra.at[pl.ds(0, half)], bbuf.at[c, 0], local_sem.at[0]),
        pltpu.make_async_copy(dbra.at[pl.ds(half, half)], bbuf.at[c, 1], local_sem.at[0]),
        pltpu.make_async_copy(eri, traw, local_sem.at[1]),
        pltpu.make_async_copy(screen, scr, local_sem.at[2]),
    ]
    kloads = [
        pltpu.make_async_copy(dket.at[:, pl.ds(u * kw, kw)], kbuf.at[r, u], local_sem.at[3])
        for u in range(KP)
    ]
    bar = pltpu.get_barrier_semaphore()

    def hello(dev):
        pl.semaphore_signal(bar, inc=1, device_id=dev, device_id_type=MESH)

    pl.when(r > 0)(lambda: hello({"row": r - 1}))
    pl.when(r < R - 1)(lambda: hello({"row": r + 1}))
    for o in range(1, C):
        hello({"col": (c + o) % C})
    hello(sib)
    for o in range(1, G):
        hello({"depth": (d + 2 * o) % Dp})
    for one in kloads:
        one.start()
    for one in loads:
        one.start()
    pl.semaphore_wait(bar, C + G - 1 + jnp.where(r > 0, 1, 0) + jnp.where(r < R - 1, 1, 0))

    def ket_send(s, u, dirn, cond):
        pl.when(cond)(lambda: remote(
            kbuf.at[s, u], kbuf.at[s, u], ks_recv.at[s, u], {"row": r - 1 + 2 * dirn}).start())

    pltpu.make_async_copy(kbuf.at[r], kbuf.at[r], local_sem.at[3]).wait()
    for u in range(KP):
        ket_send(r, u, 0, r > 0)
        ket_send(r, u, 1, r < R - 1)
    pltpu.make_async_copy(bbuf.at[c], bbuf.at[c], local_sem.at[0]).wait()
    for o in range(1, C):
        remote(bbuf.at[c, h], bbuf.at[c, h], b_recv.at[0, C - 1 - o], {"col": (c + o) % C}).start()
        sent(None, bbuf.at[c, h])
    for dirn in range(2):
        sent((r < R - 1) if dirn else (r > 0), kbuf.at[r])
    loads[2].wait()
    loads[3].wait()

    for a in range(A):
        for b in range(B):
            keep = scr[b, a] > 0
            tile = traw[a, b]
            tmat[a * PS:(a + 1) * PS, b * PS:(b + 1) * PS] = jnp.where(keep, tile, jnp.zeros_like(tile))

    def ket_block(cb):
        x = bbuf[cb].reshape(rows, db)
        res = lax.dot_general(x, tmat[...], (((0,), (0,)), ((), ())), preferred_element_type=F32)
        for j in range(per):
            for u in range(SP):
                kpart[cb * per + j, u] = res[j * dk:(j + 1) * dk, u * sw:(u + 1) * sw]

    def sum_send(t, u, dirn):
        pack(k_tx.at[t, u], kpart[t, u])
        remote(k_tx.at[t, u], k_rx.at[dirn, t, u], kr_recv.at[t + dirn, u], {"row": r - 1 + 2 * dirn}).start()

    mine = r // per == c

    def ket_ends(cb, pieces, only=None):
        for dirn in range(2):
            for j in range(per):
                t = cb * per + (per - 1 - j if dirn else j)
                go = (r == 0) & (t > r) if dirn else (r == R - 1) & (t < r)
                for u in pieces:
                    ok = go if only is None or u < SP - 1 and not only else go & (mine if only else ~mine)
                    pl.when(ok)(functools.partial(sum_send, t, u, dirn))

    first = (c * 2) // C

    def flow(late, p):
        dirn = 1 - first if late else first
        hop = jnp.where(dirn == 0, R - 1 - r, r)

        def go(p):
            k, u = p // SP, p % SP
            t = jnp.where(dirn == 0, k, R - 1 - k)
            recv(k_rx.at[dirn, t, u], kr_recv.at[t + dirn, u])
            kpart[t, u] = kpart[t, u] + unpack(k_rx.at[dirn, t, u])
            pl.when(k < R - 1 - hop)(lambda: sum_send(t, u, dirn))
        p = p - HOPS[late] * (hop - 1)
        pl.when((hop >= 1) & (p >= 0) & (p < (R - hop) * SP))(lambda: go(p))

    def slot_of(i):
        k = (i + 1) // 2
        inner = r - k if i % 2 == 1 else r + k
        inner = jnp.where(2 * r < R, 2 * r - inner, inner)
        outer = jnp.where(r > R - 1 - r, r - (i - near), r + (i - near))
        return jnp.where(i <= 2 * near, inner, outer)

    order = [slot_of(i) for i in range(R)]

    def ket_take(i, u):
        s = order[i]
        recv(kbuf.at[s, u], ks_recv.at[s, u])
        for dirn, on in ((0, (s > r) & (r > 0)), (1, (s < r) & (r < R - 1))):
            ket_send(s, u, dirn, on)
            if u == KP - 1:
                sent(on, kbuf.at[s])

    def bra_dot(i, lo, hi):
        s = order[i]
        left = jnp.concatenate([kbuf[s, u] for u in range(lo, hi)], 1)
        res = lax.dot_general(left, tmat[:, lo * kw:hi * kw], (((1,), (1,)), ((), ())), preferred_element_type=F32)
        for q in range(BP):
            for x in range(2):
                term = res[:, x * half + q * bw:x * half + (q + 1) * bw]
                bp[s, x, q] = term if lo == 0 else bp[s, x, q] + term
            if hi == KP:
                remote(bp.at[s, 1 - h, q], d1_rx.at[s, q], d1_recv.at[s, q], sib).start()
        if hi == KP:
            sent(None, bp.at[s, 1 - h])

    def bra_b(i):
        s = order[i]
        cs, j = s // per, s % per
        for q in range(BP):
            recv(d1_rx.at[s, q], d1_recv.at[s, q])
            total = bp[s, h, q] + d1_rx[s, q]
            bp[s, h, q] = total

            def go():
                pack(x_tx.at[s, q], total)
                remote(x_tx.at[s, q], x_rx.at[c, j, q], x_recv.at[(c - cs + C - 1) % C, j, q], {"col": cs}).start()
            pl.when(cs != c)(go)
        sent(cs != c, x_tx.at[s], "last")

    def bra_c(i, q):
        s = order[i]
        cs, j = s // per, s % per

        def go():
            total = bp[s, h, q]
            for o in range(1, C):
                p = (c + o) % C
                recv(x_rx.at[p, j, q], x_recv.at[o - 1, j, q])
                total = total + unpack(x_rx.at[p, j, q])
            pack(y_rx.at[j, g, q], total)
            for o in range(1, G):
                remote(y_rx.at[j, g, q], y_rx.at[j, g, q], y_recv.at[j, G - 1 - o, q],
                       {"depth": (d + 2 * o) % Dp}).start()
        pl.when(cs == c)(go)

    def out_at(j, q, side):
        return pl.ds(pl.multiple_of(j * dk, 8), dk), pl.ds(pl.multiple_of(side * half + q * bw, 128), bw)

    def bra_d(i, q):
        s = order[i]
        cs, j = s // per, s % per

        def go():
            for o in range(1, G):
                p = (g + o) % G
                recv(y_rx.at[j, p, q], y_recv.at[j, o - 1, q])
            total = unpack(y_rx.at[j, 0, q])
            for p in range(1, G):
                total = total + unpack(y_rx.at[j, p, q])
            fin[j, q] = total
            at = out_at(j, q, h)
            remote(fin.at[j, q], out_b.at[at], f_recv, sib).start()
            out_b[at] = total
        pl.when(cs == c)(go)

    def bra_e():
        recv(fin, f_recv)

    others = [(c + o) % C for o in range(1, C)]

    def bra_forward():
        for o, p in enumerate(others):
            recv(bbuf.at[p, h], b_recv.at[0, o])
            remote(bbuf.at[p, h], bbuf.at[p, h], b_recv.at[1, o], sib).start()
            sent(None, bbuf.at[p, h])

    def ket_others():
        for o, p in enumerate(others):
            recv(bbuf.at[p, 1 - h], b_recv.at[1, o])
            ket_block(p)
            ket_ends(p, range(SP))

    def take_dot(i, lo, hi, *more):
        for u in range(lo, hi):
            for k in (i, *more):
                ket_take(k, u)
        bra_dot(i, lo, hi)

    mid = KP // 2

    def start_edge():
        ket_ends(c, range(SP), False)
        bra_dot(0, 0, KP)
        take_dot(1, 0, mid)
        take_dot(1, mid, KP)
        bra_forward()
        bra_b(0)
        ket_others()
        ket_ends(c, [SP - 1], True)
        bra_b(1)
        for i in range(2, R):
            if i > 2:
                bra_b(i - 1)
                for q in range(BP):
                    bra_c(i - 3, q)
            take_dot(i, 0, mid)
            take_dot(i, mid, KP - 1)
            take_dot(i, KP - 1, KP)
        for q in range(BP):
            bra_c(R - 2, q)
        bra_b(R - 1)
        for q in range(BP):
            bra_c(R - 3, q)
        return R - 1

    def start_inside():
        bra_dot(0, 0, KP)
        take_dot(1, 0, mid, 2)
        take_dot(1, mid, KP, 2)
        bra_b(0)
        bra_dot(2, 0, KP)
        bra_forward()
        take_dot(3, 0, mid)
        bra_b(1)
        take_dot(3, mid, KP)
        ket_others()
        bra_b(2)
        for i in range(4, R):
            take_dot(i, 0, KP)
            bra_b(i - 1)
        return 0

    def finish(kind, done):
        tail = [] if kind == "edge" else [(12.1, bra_b, (R - 1,))]
        for late in (False, True):
            lag = HOPS[late]
            if kind == "edge":
                steps = range(lag * (R - 2), lag * (R - 2) + SP)
            else:
                steps = range(max((R - hop) * SP + lag * (hop - 1) for hop in range(1, R - 1)))
            for p in steps:
                tail.append(((13.5 if late else 8.5) + 1.05 * p, flow, (late, p)))
        if kind == "edge":
            when_bra = {0: (12.9, 16.5, 1.0), 1: (15.5, 19.2, 1.0), 2: (15.6, 22.3, 0.1), 3: (19.0, 22.5, 1.05)}
        else:
            when_bra = {0: (12.4, 16.5, 0.6), 1: (13.4, 17.1, 1.0), 2: (16.0, 20.7, 0.5), 3: (16.0, 20.1, 1.0)}
        for i in range(R):
            col_at, depth_at, step = when_bra.get(i, (19.0 + 4 * (i - 3), 22.5 + 4 * (i - 3), 1.05))
            for q in range(BP):
                if i >= done:
                    tail.append((col_at + step * q, bra_c, (i, q)))
                tail.append((depth_at + step * q, bra_d, (i, q)))
        tail.sort(key=lambda x: x[0])
        first_done = last_done = False
        for at, fn, args in tail:
            if at > 19 and not first_done:
                flush("first")
                first_done = True
            if at > 23.6 and not last_done:
                flush("last")
                last_done = True
            fn(*args)
        bra_e()
        for u in range(SP):
            out_k[:, u * sw:(u + 1) * sw] = kpart[r, u]
        pending["last"].clear()
        for t in range(R):
            sent(t != r, k_tx.at[t], "last")
        for j in range(per):
            for o in range(1, G):
                sent(None, y_rx.at[j, g], "last")
            sent(None, fin.at[j], "last")
        flush("last")

    ket_block(c)
    front = list(pending["first"])

    def run(kind):
        pending["first"], pending["last"] = list(front), []
        finish(kind, start_edge() if kind == "edge" else start_inside())

    pl.when(near == 0)(lambda: run("edge"))
    pl.when(near > 0)(lambda: run("inside"))


def store(bra_t, ket_t, bra, ket, turned, sem):
    kets = pltpu.make_async_copy(ket_t, ket, sem.at[0])
    kets.start()
    size = turned.shape[0] // STORES
    copies = []
    for i in range(STORES):
        at = pl.ds(i * size, size)
        turned[at] = bra_t[:, at].T
        copies.append(pltpu.make_async_copy(turned.at[at], bra.at[at], sem.at[1 + i]))
        copies[-1].start()
    for one in [kets, *copies]:
        one.wait()


def body(sizes, eri_tiles, screen, density_bra, density_ket):
    R, C, Dp = sizes
    A, B, PS, _ = eri_tiles.shape
    rows, cols = A * PS, B * PS
    db, dk = density_bra.shape[1], density_ket.shape[1]
    per, G, half = R // C, Dp // 2, rows // 2
    DMA = pltpu.SemaphoreType.DMA
    hbm = pl.BlockSpec(memory_space=pltpu.HBM)
    vm = pl.BlockSpec(memory_space=pltpu.VMEM)
    piece, coded = (dk, half // BP), (dk, half // BP * 3 // 2)
    out_b, out_k = pl.pallas_call(
        functools.partial(kernel, sizes),
        out_shape=(jax.ShapeDtypeStruct((db, rows), F32), jax.ShapeDtypeStruct((dk, cols), F32)),
        in_specs=[hbm, hbm, hbm, hbm],
        out_specs=(vm, vm),
        scratch_shapes=[
            pltpu.SMEM((B, A), jnp.int32),
            pltpu.VMEM((A, B, PS, PS), BF16),
            pltpu.VMEM((rows, cols), BF16),
            pltpu.VMEM((R, KP, dk, cols // KP), BF16),
            pltpu.VMEM((C, 2, half, db), BF16),
            pltpu.VMEM((R, SP, dk, cols // SP), F32),
            pltpu.VMEM((R, SP, dk, cols // SP * 3 // 2), BF16),
            pltpu.VMEM((2, R, SP, dk, cols // SP * 3 // 2), BF16),
            pltpu.VMEM((R, 2, BP, *piece), F32),
            pltpu.VMEM((R, BP, *piece), F32),
            pltpu.VMEM((R, BP, *coded), BF16),
            pltpu.VMEM((C, per, BP, *coded), BF16),
            pltpu.VMEM((per, G, BP, *coded), BF16),
            pltpu.VMEM((per, BP, *piece), F32),
            DMA((4,)), DMA, DMA((R, KP)), DMA((2, C - 1)), DMA((R + 1, SP)),
            DMA((R, BP)), DMA((C - 1, per, BP)), DMA((per, G - 1, BP)), DMA,
        ],
        compiler_params=pltpu.CompilerParams(
            collective_id=0, has_side_effects=True, vmem_limit_bytes=28 * 1024 * 1024),
    )(*(pltpu.with_memory_space_constraint(x, pltpu.HBM) for x in (eri_tiles, screen.T, density_bra, density_ket.T)))
    bra, ket = pl.pallas_call(
        store,
        out_shape=(jax.ShapeDtypeStruct((rows, db), F32), jax.ShapeDtypeStruct((dk, cols), F32)),
        in_specs=[vm, vm],
        out_specs=(hbm, hbm),
        scratch_shapes=[pltpu.VMEM((rows, db), F32), DMA((1 + STORES,))],
        compiler_params=pltpu.CompilerParams(vmem_limit_bytes=4 * 1024 * 1024),
    )(out_b, out_k)
    return bra, ket.T


def solution(mesh):
    sizes = (mesh.shape["row"], mesh.shape["col"], mesh.shape["depth"])
    return jax.shard_map(
        functools.partial(body, sizes),
        mesh=mesh,
        in_specs=(
            P("row", ("col", "depth"), None, None),
            P("row", ("col", "depth")),
            P("row", "col"),
            P(("col", "depth"), "row"),
        ),
        out_specs=(P("row", "col"), P(("col", "depth"), "row")),
        check_vma=False,
    )
```

```python
import functools

import jax
import jax.numpy as jnp
from jax import lax
from jax.experimental import pallas as pl
from jax.experimental.pallas import tpu as pltpu
from jax.sharding import PartitionSpec as P

MESH = pl.DeviceIdType.MESH
F32 = jnp.float32
BF16 = jnp.bfloat16
STEPS = 7 * 2.0**8
KP = 4
SP = 4
HOPS = (6, 4)
STORES = 4
BP = 6
B0 = 2


def pack(ref, v):
    w = v.shape[1]
    top = v.astype(BF16)
    near = top.astype(F32)
    rest = jnp.round((v - near) / jnp.where(near == 0, 1.0, near) * STEPS)
    ref[:, :w] = top
    ref[:, w:] = (rest[:, :w // 2] * 16 + rest[:, w // 2:]).astype(BF16)


def unpack(ref):
    w = ref.shape[1] * 2 // 3
    near = ref[:, :w].astype(F32)
    both = ref[:, w:].astype(F32)
    high = jnp.round(both * (1 / 16))
    rest = jnp.concatenate([high, both - high * 16], 1)
    return near + near * rest * (1 / STEPS)


def kernel(
    sizes, eri, screen, dbra, dket, out_b, out_k,
    scr, traw, tmat, kbuf, bbuf, kpart, k_tx, k_rx, bp, d1_rx, x_tx, x_rx, y_rx, fin,
    local_sem, send_sem, ks_recv, b_recv, kr_recv, d1_recv, x_recv, y_recv, f_recv,
):
    R, C, Dp = sizes
    per = R // C
    G = Dp // 2
    r, c, d = lax.axis_index("row"), lax.axis_index("col"), lax.axis_index("depth")
    h = d % 2
    g = d // 2
    sib = {"depth": d + 1 - 2 * h}
    A, B, PS = eri.shape[0], eri.shape[1], eri.shape[2]
    rows, cols = A * PS, B * PS
    dk, kw = kbuf.shape[2], kbuf.shape[3]
    sw = kpart.shape[3]
    db = bbuf.shape[3]
    half = rows // 2
    bw = rows // BP
    B1 = BP - B0
    near = jnp.minimum(r, R - 1 - r)
    pending = {"first": [], "last": []}

    def when(cond, fn):
        if cond is None:
            fn()
        else:
            pl.when(cond)(fn)

    def remote(src, dst, rsem, dev):
        return pltpu.make_async_remote_copy(
            src_ref=src, dst_ref=dst, send_sem=send_sem, recv_sem=rsem, device_id=dev, device_id_type=MESH)

    def sent(cond, src, group="first"):
        pending[group].append((cond, lambda: remote(src, src, send_sem, sib).wait_send()))

    def own(q, fn):
        if q < min(B0, B1):
            fn()
        else:
            pl.when(h == (0 if q < B0 else 1))(fn)

    def sent_own(cond, ref, group="first"):
        for x, n in ((0, B0), (1, B1)):
            mine = h == x
            sent(mine if cond is None else mine & cond, ref.at[pl.ds(0, n)], group)

    def recv(dst, rsem):
        remote(dst, dst, rsem, sib).wait_recv()

    def flush(group):
        for cond, wait in pending[group]:
            when(cond, wait)

    loads = [
        pltpu.make_async_copy(dbra.at[pl.ds(0, half)], bbuf.at[c, 0], local_sem.at[0]),
        pltpu.make_async_copy(dbra.at[pl.ds(half, half)], bbuf.at[c, 1], local_sem.at[0]),
        pltpu.make_async_copy(eri, traw, local_sem.at[1]),
        pltpu.make_async_copy(screen, scr, local_sem.at[2]),
    ]
    kloads = [
        pltpu.make_async_copy(dket.at[:, pl.ds(u * kw, kw)], kbuf.at[r, u], local_sem.at[3])
        for u in range(KP)
    ]
    bar = pltpu.get_barrier_semaphore()

    def hello(dev):
        pl.semaphore_signal(bar, inc=1, device_id=dev, device_id_type=MESH)

    pl.when(r > 0)(lambda: hello({"row": r - 1}))
    pl.when(r < R - 1)(lambda: hello({"row": r + 1}))
    for o in range(1, C):
        hello({"col": (c + o) % C})
    hello(sib)
    for o in range(1, G):
        hello({"depth": (d + 2 * o) % Dp})
    for one in kloads:
        one.start()
    for one in loads:
        one.start()
    pl.semaphore_wait(bar, C + G - 1 + jnp.where(r > 0, 1, 0) + jnp.where(r < R - 1, 1, 0))

    def ket_send(s, u, dirn, cond):
        pl.when(cond)(lambda: remote(
            kbuf.at[s, u], kbuf.at[s, u], ks_recv.at[s, u], {"row": r - 1 + 2 * dirn}).start())

    pltpu.make_async_copy(kbuf.at[r], kbuf.at[r], local_sem.at[3]).wait()
    for u in range(KP):
        ket_send(r, u, 0, r > 0)
        ket_send(r, u, 1, r < R - 1)
    pltpu.make_async_copy(bbuf.at[c], bbuf.at[c], local_sem.at[0]).wait()
    for o in range(1, C):
        remote(bbuf.at[c, h], bbuf.at[c, h], b_recv.at[0, C - 1 - o], {"col": (c + o) % C}).start()
        sent(None, bbuf.at[c, h])
    for dirn in range(2):
        sent((r < R - 1) if dirn else (r > 0), kbuf.at[r])
    loads[2].wait()
    loads[3].wait()

    for a in range(A):
        for b in range(B):
            keep = scr[b, a] > 0
            tile = traw[a, b]
            tmat[a * PS:(a + 1) * PS, b * PS:(b + 1) * PS] = jnp.where(keep, tile, jnp.zeros_like(tile))

    def ket_block(cb):
        x = bbuf[cb].reshape(rows, db)
        res = lax.dot_general(x, tmat[...], (((0,), (0,)), ((), ())), preferred_element_type=F32)
        for j in range(per):
            for u in range(SP):
                kpart[cb * per + j, u] = res[j * dk:(j + 1) * dk, u * sw:(u + 1) * sw]

    def sum_send(t, u, dirn):
        pack(k_tx.at[t, u], kpart[t, u])
        remote(k_tx.at[t, u], k_rx.at[dirn, t, u], kr_recv.at[t + dirn, u], {"row": r - 1 + 2 * dirn}).start()

    mine = r // per == c

    def ket_ends(cb, pieces, only=None):
        for dirn in range(2):
            for j in range(per):
                t = cb * per + (per - 1 - j if dirn else j)
                go = (r == 0) & (t > r) if dirn else (r == R - 1) & (t < r)
                for u in pieces:
                    ok = go if only is None or u < SP - 1 and not only else go & (mine if only else ~mine)
                    pl.when(ok)(functools.partial(sum_send, t, u, dirn))

    first = (c * 2) // C

    def flow(late, p):
        dirn = 1 - first if late else first
        hop = jnp.where(dirn == 0, R - 1 - r, r)

        def go(p):
            k, u = p // SP, p % SP
            t = jnp.where(dirn == 0, k, R - 1 - k)
            recv(k_rx.at[dirn, t, u], kr_recv.at[t + dirn, u])
            kpart[t, u] = kpart[t, u] + unpack(k_rx.at[dirn, t, u])
            pl.when(k < R - 1 - hop)(lambda: sum_send(t, u, dirn))
        p = p - HOPS[late] * (hop - 1)
        pl.when((hop >= 1) & (p >= 0) & (p < (R - hop) * SP))(lambda: go(p))

    def slot_of(i):
        k = (i + 1) // 2
        inner = r - k if i % 2 == 1 else r + k
        inner = jnp.where(2 * r < R, 2 * r - inner, inner)
        outer = jnp.where(r > R - 1 - r, r - (i - near), r + (i - near))
        return jnp.where(i <= 2 * near, inner, outer)

    order = [slot_of(i) for i in range(R)]

    def ket_take(i, u):
        s = order[i]
        recv(kbuf.at[s, u], ks_recv.at[s, u])
        for dirn, on in ((0, (s > r) & (r > 0)), (1, (s < r) & (r < R - 1))):
            ket_send(s, u, dirn, on)
            if u == KP - 1:
                sent(on, kbuf.at[s])

    def bra_dot(i, lo, hi):
        s = order[i]
        left = jnp.concatenate([kbuf[s, u] for u in range(lo, hi)], 1)
        res = lax.dot_general(left, tmat[:, lo * kw:hi * kw], (((1,), (1,)), ((), ())), preferred_element_type=F32)
        for p in range(BP):
            term = res[:, p * bw:(p + 1) * bw]
            bp[s, p] = term if lo == 0 else bp[s, p] + term
        if hi == KP:
            for p in range(BP):
                q = p if p < B0 else p - B0
                pl.when(h == (1 if p < B0 else 0))(lambda: remote(
                    bp.at[s, p], d1_rx.at[s, q], d1_recv.at[s, q], sib).start())
            sent(h == 1, bp.at[s, pl.ds(0, B0)])
            sent(h == 0, bp.at[s, pl.ds(B0, B1)])

    def bra_b(i):
        s = order[i]
        cs, j = s // per, s % per

        def piece(q):
            p = q + B0 * h
            recv(d1_rx.at[s, q], d1_recv.at[s, q])
            total = bp[s, p] + d1_rx[s, q]
            bp[s, p] = total

            def go():
                pack(x_tx.at[s, q], total)
                remote(x_tx.at[s, q], x_rx.at[c, j, q], x_recv.at[(c - cs + C - 1) % C, j, q], {"col": cs}).start()
            pl.when(cs != c)(go)
        for q in range(max(B0, B1)):
            own(q, functools.partial(piece, q))
        sent_own(cs != c, x_tx.at[s], "last")

    def bra_c(i, q):
        s = order[i]
        cs, j = s // per, s % per

        def go():
            total = bp[s, q + B0 * h]
            for o in range(1, C):
                p = (c + o) % C
                recv(x_rx.at[p, j, q], x_recv.at[o - 1, j, q])
                total = total + unpack(x_rx.at[p, j, q])
            pack(y_rx.at[j, g, q], total)
            for o in range(1, G):
                remote(y_rx.at[j, g, q], y_rx.at[j, g, q], y_recv.at[j, G - 1 - o, q],
                       {"depth": (d + 2 * o) % Dp}).start()
        own(q, lambda: pl.when(cs == c)(go))

    def bra_d(i, q):
        s = order[i]
        cs, j = s // per, s % per

        def go():
            for o in range(1, G):
                p = (g + o) % G
                recv(y_rx.at[j, p, q], y_recv.at[j, o - 1, q])
            total = unpack(y_rx.at[j, 0, q])
            for p in range(1, G):
                total = total + unpack(y_rx.at[j, p, q])
            fin[j, q] = total
            at = pl.ds(pl.multiple_of(j * dk, 8), dk), pl.ds(pl.multiple_of((q + B0 * h) * bw, 128), bw)
            remote(fin.at[j, q], out_b.at[at], f_recv, sib).start()
            out_b[at] = total
        own(q, lambda: pl.when(cs == c)(go))

    def bra_e():
        for x, n in ((1, B0), (0, B1)):
            pl.when(h == x)(lambda: recv(fin.at[:, pl.ds(0, n)], f_recv))

    others = [(c + o) % C for o in range(1, C)]

    def bra_forward():
        for o, p in enumerate(others):
            recv(bbuf.at[p, h], b_recv.at[0, o])
            remote(bbuf.at[p, h], bbuf.at[p, h], b_recv.at[1, o], sib).start()
            sent(None, bbuf.at[p, h])

    def ket_others():
        for o, p in enumerate(others):
            recv(bbuf.at[p, 1 - h], b_recv.at[1, o])
            ket_block(p)
            ket_ends(p, range(SP))

    def take_dot(i, lo, hi, *more):
        for u in range(lo, hi):
            for k in (i, *more):
                ket_take(k, u)
        bra_dot(i, lo, hi)

    mid = KP // 2

    def start_edge():
        ket_ends(c, range(SP), False)
        bra_dot(0, 0, KP)
        take_dot(1, 0, mid)
        take_dot(1, mid, KP)
        bra_forward()
        bra_b(0)
        ket_others()
        ket_ends(c, [SP - 1], True)
        bra_b(1)
        for i in range(2, R):
            if i > 2:
                bra_b(i - 1)
                for q in range(max(B0, B1)):
                    bra_c(i - 3, q)
            take_dot(i, 0, mid)
            take_dot(i, mid, KP - 1)
            take_dot(i, KP - 1, KP)
        for q in range(max(B0, B1)):
            bra_c(R - 2, q)
        bra_b(R - 1)
        for q in range(max(B0, B1)):
            bra_c(R - 3, q)
        return R - 1

    def start_inside():
        bra_dot(0, 0, KP)
        take_dot(1, 0, mid, 2)
        take_dot(1, mid, KP, 2)
        bra_b(0)
        bra_dot(2, 0, KP)
        bra_forward()
        take_dot(3, 0, mid)
        bra_b(1)
        take_dot(3, mid, KP)
        ket_others()
        bra_b(2)
        for i in range(4, R):
            take_dot(i, 0, KP)
            bra_b(i - 1)
        return 0

    def finish(kind, done):
        tail = [] if kind == "edge" else [(12.1, bra_b, (R - 1,))]
        for late in (False, True):
            lag = HOPS[late]
            if kind == "edge":
                steps = range(lag * (R - 2), lag * (R - 2) + SP)
            else:
                steps = range(max((R - hop) * SP + lag * (hop - 1) for hop in range(1, R - 1)))
            for p in steps:
                tail.append(((13.5 if late else 8.5) + 1.05 * p, flow, (late, p)))
        if kind == "edge":
            when_bra = {0: (12.9, 16.5, 1.0), 1: (15.5, 19.2, 1.0), 2: (15.6, 22.3, 0.1), 3: (19.0, 22.5, 1.05)}
        else:
            when_bra = {0: (12.4, 16.5, 0.6), 1: (13.4, 17.1, 1.0), 2: (16.0, 20.7, 0.5), 3: (16.0, 20.1, 1.0)}
        for i in range(R):
            col_at, depth_at, step = when_bra.get(i, (19.0 + 4 * (i - 3), 22.5 + 4 * (i - 3), 1.05))
            for q in range(max(B0, B1)):
                if i >= done:
                    tail.append((col_at + step * q, bra_c, (i, q)))
                tail.append((depth_at + step * q, bra_d, (i, q)))
        tail.sort(key=lambda x: x[0])
        first_done = last_done = False
        for at, fn, args in tail:
            if at > 19 and not first_done:
                flush("first")
                first_done = True
            if at > 23.6 and not last_done:
                flush("last")
                last_done = True
            fn(*args)
        bra_e()
        for u in range(SP):
            out_k[:, u * sw:(u + 1) * sw] = kpart[r, u]
        pending["last"].clear()
        for t in range(R):
            sent(t != r, k_tx.at[t], "last")
        for j in range(per):
            for o in range(1, G):
                sent_own(None, y_rx.at[j, g], "last")
            sent_own(None, fin.at[j], "last")
        flush("last")

    ket_block(c)
    front = list(pending["first"])

    def run(kind):
        pending["first"], pending["last"] = list(front), []
        finish(kind, start_edge() if kind == "edge" else start_inside())

    pl.when(near == 0)(lambda: run("edge"))
    pl.when(near > 0)(lambda: run("inside"))


def store(bra_t, ket_t, bra, ket, turned, sem):
    kets = pltpu.make_async_copy(ket_t, ket, sem.at[0])
    kets.start()
    size = turned.shape[0] // STORES
    copies = []
    for i in range(STORES):
        at = pl.ds(i * size, size)
        turned[at] = bra_t[:, at].T
        copies.append(pltpu.make_async_copy(turned.at[at], bra.at[at], sem.at[1 + i]))
        copies[-1].start()
    for one in [kets, *copies]:
        one.wait()


def body(sizes, eri_tiles, screen, density_bra, density_ket):
    R, C, Dp = sizes
    A, B, PS, _ = eri_tiles.shape
    rows, cols = A * PS, B * PS
    db, dk = density_bra.shape[1], density_ket.shape[1]
    per, G, half = R // C, Dp // 2, rows // 2
    DMA = pltpu.SemaphoreType.DMA
    hbm = pl.BlockSpec(memory_space=pltpu.HBM)
    vm = pl.BlockSpec(memory_space=pltpu.VMEM)
    piece, coded, most = (dk, rows // BP), (dk, rows // BP * 3 // 2), max(B0, BP - B0)
    out_b, out_k = pl.pallas_call(
        functools.partial(kernel, sizes),
        out_shape=(jax.ShapeDtypeStruct((db, rows), F32), jax.ShapeDtypeStruct((dk, cols), F32)),
        in_specs=[hbm, hbm, hbm, hbm],
        out_specs=(vm, vm),
        scratch_shapes=[
            pltpu.SMEM((B, A), jnp.int32),
            pltpu.VMEM((A, B, PS, PS), BF16),
            pltpu.VMEM((rows, cols), BF16),
            pltpu.VMEM((R, KP, dk, cols // KP), BF16),
            pltpu.VMEM((C, 2, half, db), BF16),
            pltpu.VMEM((R, SP, dk, cols // SP), F32),
            pltpu.VMEM((R, SP, dk, cols // SP * 3 // 2), BF16),
            pltpu.VMEM((2, R, SP, dk, cols // SP * 3 // 2), BF16),
            pltpu.VMEM((R, BP, *piece), F32),
            pltpu.VMEM((R, most, *piece), F32),
            pltpu.VMEM((R, most, *coded), BF16),
            pltpu.VMEM((C, per, most, *coded), BF16),
            pltpu.VMEM((per, G, most, *coded), BF16),
            pltpu.VMEM((per, most, *piece), F32),
            DMA((4,)), DMA, DMA((R, KP)), DMA((2, C - 1)), DMA((R + 1, SP)),
            DMA((R, most)), DMA((C - 1, per, most)), DMA((per, G - 1, most)), DMA,
        ],
        compiler_params=pltpu.CompilerParams(
            collective_id=0, has_side_effects=True, vmem_limit_bytes=28 * 1024 * 1024),
    )(*(pltpu.with_memory_space_constraint(x, pltpu.HBM) for x in (eri_tiles, screen.T, density_bra, density_ket.T)))
    bra, ket = pl.pallas_call(
        store,
        out_shape=(jax.ShapeDtypeStruct((rows, db), F32), jax.ShapeDtypeStruct((dk, cols), F32)),
        in_specs=[vm, vm],
        out_specs=(hbm, hbm),
        scratch_shapes=[pltpu.VMEM((rows, db), F32), DMA((1 + STORES,))],
        compiler_params=pltpu.CompilerParams(vmem_limit_bytes=4 * 1024 * 1024),
    )(out_b, out_k)
    return bra, ket.T


def solution(mesh):
    sizes = (mesh.shape["row"], mesh.shape["col"], mesh.shape["depth"])
    return jax.shard_map(
        functools.partial(body, sizes),
        mesh=mesh,
        in_specs=(
            P("row", ("col", "depth"), None, None),
            P("row", ("col", "depth")),
            P("row", "col"),
            P(("col", "depth"), "row"),
        ),
        out_specs=(P("row", "col"), P(("col", "depth"), "row")),
        check_vma=False,
    )
```

```python
import functools

import jax
import jax.numpy as jnp
from jax import lax
from jax.experimental import pallas as pl
from jax.experimental.pallas import tpu as pltpu
from jax.sharding import PartitionSpec as P

MESH = pl.DeviceIdType.MESH
F32 = jnp.float32
BF16 = jnp.bfloat16
STEPS = 7 * 2.0**8
TINY = 1e-36
KP = 4
SP = 4
HOPS = (6, 4)
STORES = 4
BP = 6
B0 = 2


def pack(ref, v):
    w = v.shape[1]
    top = v.astype(BF16)
    near = top.astype(F32)
    rest = jnp.round((v - near) / jnp.where(jnp.abs(near) < TINY, 1.0, near) * STEPS)
    ref[:, :w] = top
    ref[:, w:] = (rest[:, :w // 2] * 16 + rest[:, w // 2:]).astype(BF16)


def unpack(ref):
    w = ref.shape[1] * 2 // 3
    near = ref[:, :w].astype(F32)
    both = ref[:, w:].astype(F32)
    high = jnp.round(both * (1 / 16))
    rest = jnp.concatenate([high, both - high * 16], 1)
    return near + near * rest * (1 / STEPS)


def kernel(
    sizes, eri, screen, dbra, dket, out_b, out_k,
    scr, traw, tmat, kbuf, bbuf, kpart, k_tx, k_rx, bp, d1_rx, x_tx, x_rx, y_rx, fin,
    local_sem, send_sem, ks_recv, b_recv, kr_recv, d1_recv, x_recv, y_recv, f_recv,
):
    R, C, Dp = sizes
    per = R // C
    G = Dp // 2
    r, c, d = lax.axis_index("row"), lax.axis_index("col"), lax.axis_index("depth")
    h = d % 2
    g = d // 2
    sib = {"depth": d + 1 - 2 * h}
    A, B, PS = eri.shape[0], eri.shape[1], eri.shape[2]
    rows, cols = A * PS, B * PS
    dk, kw = kbuf.shape[2], kbuf.shape[3]
    sw = kpart.shape[3]
    db = bbuf.shape[3]
    half = rows // 2
    bw = rows // BP
    B1 = BP - B0
    near = jnp.minimum(r, R - 1 - r)
    pending = {"first": [], "last": []}

    def when(cond, fn):
        if cond is None:
            fn()
        else:
            pl.when(cond)(fn)

    def remote(src, dst, rsem, dev):
        return pltpu.make_async_remote_copy(
            src_ref=src, dst_ref=dst, send_sem=send_sem, recv_sem=rsem, device_id=dev, device_id_type=MESH)

    def sent(cond, src, group="first"):
        pending[group].append((cond, lambda: remote(src, src, send_sem, sib).wait_send()))

    def own(q, fn):
        if q < min(B0, B1):
            fn()
        else:
            pl.when(h == (0 if q < B0 else 1))(fn)

    def sent_own(cond, ref, group="first"):
        for x, n in ((0, B0), (1, B1)):
            mine = h == x
            sent(mine if cond is None else mine & cond, ref.at[pl.ds(0, n)], group)

    def recv(dst, rsem):
        remote(dst, dst, rsem, sib).wait_recv()

    def flush(group):
        for cond, wait in pending[group]:
            when(cond, wait)

    loads = [
        pltpu.make_async_copy(dbra.at[pl.ds(0, half)], bbuf.at[c, 0], local_sem.at[0]),
        pltpu.make_async_copy(dbra.at[pl.ds(half, half)], bbuf.at[c, 1], local_sem.at[0]),
        pltpu.make_async_copy(eri, traw, local_sem.at[1]),
        pltpu.make_async_copy(screen, scr, local_sem.at[2]),
    ]
    kloads = [
        pltpu.make_async_copy(dket.at[:, pl.ds(u * kw, kw)], kbuf.at[r, u], local_sem.at[3])
        for u in range(KP)
    ]
    bar = pltpu.get_barrier_semaphore()

    def hello(dev):
        pl.semaphore_signal(bar, inc=1, device_id=dev, device_id_type=MESH)

    pl.when(r > 0)(lambda: hello({"row": r - 1}))
    pl.when(r < R - 1)(lambda: hello({"row": r + 1}))
    for o in range(1, C):
        hello({"col": (c + o) % C})
    hello(sib)
    for o in range(1, G):
        hello({"depth": (d + 2 * o) % Dp})
    for one in kloads:
        one.start()
    for one in loads:
        one.start()
    pl.semaphore_wait(bar, C + G - 1 + jnp.where(r > 0, 1, 0) + jnp.where(r < R - 1, 1, 0))

    def ket_send(s, u, dirn, cond):
        pl.when(cond)(lambda: remote(
            kbuf.at[s, u], kbuf.at[s, u], ks_recv.at[s, u], {"row": r - 1 + 2 * dirn}).start())

    pltpu.make_async_copy(kbuf.at[r], kbuf.at[r], local_sem.at[3]).wait()
    for u in range(KP):
        ket_send(r, u, 0, r > 0)
        ket_send(r, u, 1, r < R - 1)
    pltpu.make_async_copy(bbuf.at[c], bbuf.at[c], local_sem.at[0]).wait()
    for o in range(1, C):
        remote(bbuf.at[c, h], bbuf.at[c, h], b_recv.at[0, C - 1 - o], {"col": (c + o) % C}).start()
        sent(None, bbuf.at[c, h])
    for dirn in range(2):
        sent((r < R - 1) if dirn else (r > 0), kbuf.at[r])
    loads[2].wait()
    loads[3].wait()

    for a in range(A):
        for b in range(B):
            keep = scr[b, a] > 0
            tile = traw[a, b]
            tmat[a * PS:(a + 1) * PS, b * PS:(b + 1) * PS] = jnp.where(keep, tile, jnp.zeros_like(tile))

    def ket_block(cb):
        x = bbuf[cb].reshape(rows, db)
        res = lax.dot_general(x, tmat[...], (((0,), (0,)), ((), ())), preferred_element_type=F32)
        for j in range(per):
            for u in range(SP):
                kpart[cb * per + j, u] = res[j * dk:(j + 1) * dk, u * sw:(u + 1) * sw]

    def sum_send(t, u, dirn):
        pack(k_tx.at[t, u], kpart[t, u])
        remote(k_tx.at[t, u], k_rx.at[dirn, t, u], kr_recv.at[t + dirn, u], {"row": r - 1 + 2 * dirn}).start()

    mine = r // per == c

    def ket_ends(cb, pieces, only=None):
        for dirn in range(2):
            for j in range(per):
                t = cb * per + (per - 1 - j if dirn else j)
                go = (r == 0) & (t > r) if dirn else (r == R - 1) & (t < r)
                for u in pieces:
                    ok = go if only is None or u < SP - 1 and not only else go & (mine if only else ~mine)
                    pl.when(ok)(functools.partial(sum_send, t, u, dirn))

    first = (c * 2) // C

    def flow(late, p):
        dirn = 1 - first if late else first
        hop = jnp.where(dirn == 0, R - 1 - r, r)

        def go(p):
            k, u = p // SP, p % SP
            t = jnp.where(dirn == 0, k, R - 1 - k)
            recv(k_rx.at[dirn, t, u], kr_recv.at[t + dirn, u])
            kpart[t, u] = kpart[t, u] + unpack(k_rx.at[dirn, t, u])
            pl.when(k < R - 1 - hop)(lambda: sum_send(t, u, dirn))
        p = p - HOPS[late] * (hop - 1)
        pl.when((hop >= 1) & (p >= 0) & (p < (R - hop) * SP))(lambda: go(p))

    def slot_of(i):
        k = (i + 1) // 2
        inner = r - k if i % 2 == 1 else r + k
        inner = jnp.where(2 * r < R, 2 * r - inner, inner)
        outer = jnp.where(r > R - 1 - r, r - (i - near), r + (i - near))
        return jnp.where(i <= 2 * near, inner, outer)

    order = [slot_of(i) for i in range(R)]

    def ket_take(i, u):
        s = order[i]
        recv(kbuf.at[s, u], ks_recv.at[s, u])
        for dirn, on in ((0, (s > r) & (r > 0)), (1, (s < r) & (r < R - 1))):
            ket_send(s, u, dirn, on)
            if u == KP - 1:
                sent(on, kbuf.at[s])

    def bra_dot(i, lo, hi):
        s = order[i]
        left = jnp.concatenate([kbuf[s, u] for u in range(lo, hi)], 1)
        res = lax.dot_general(left, tmat[:, lo * kw:hi * kw], (((1,), (1,)), ((), ())), preferred_element_type=F32)
        for p in range(BP):
            term = res[:, p * bw:(p + 1) * bw]
            bp[s, p] = term if lo == 0 else bp[s, p] + term
        if hi == KP:
            for p in range(BP):
                q = p if p < B0 else p - B0
                pl.when(h == (1 if p < B0 else 0))(lambda: remote(
                    bp.at[s, p], d1_rx.at[s, q], d1_recv.at[s, q], sib).start())
            sent(h == 1, bp.at[s, pl.ds(0, B0)])
            sent(h == 0, bp.at[s, pl.ds(B0, B1)])

    def bra_b(i):
        s = order[i]
        cs, j = s // per, s % per

        def piece(q):
            p = q + B0 * h
            recv(d1_rx.at[s, q], d1_recv.at[s, q])
            total = bp[s, p] + d1_rx[s, q]
            bp[s, p] = total

            def go():
                pack(x_tx.at[s, q], total)
                remote(x_tx.at[s, q], x_rx.at[c, j, q], x_recv.at[(c - cs + C - 1) % C, j, q], {"col": cs}).start()
            pl.when(cs != c)(go)
        for q in range(max(B0, B1)):
            own(q, functools.partial(piece, q))
        sent_own(cs != c, x_tx.at[s], "last")

    def bra_c(i, q):
        s = order[i]
        cs, j = s // per, s % per

        def go():
            total = bp[s, q + B0 * h]
            for o in range(1, C):
                p = (c + o) % C
                recv(x_rx.at[p, j, q], x_recv.at[o - 1, j, q])
                total = total + unpack(x_rx.at[p, j, q])
            pack(y_rx.at[j, g, q], total)
            for o in range(1, G):
                remote(y_rx.at[j, g, q], y_rx.at[j, g, q], y_recv.at[j, G - 1 - o, q],
                       {"depth": (d + 2 * o) % Dp}).start()
        own(q, lambda: pl.when(cs == c)(go))

    def bra_d(i, q):
        s = order[i]
        cs, j = s // per, s % per

        def go():
            for o in range(1, G):
                p = (g + o) % G
                recv(y_rx.at[j, p, q], y_recv.at[j, o - 1, q])
            total = unpack(y_rx.at[j, 0, q])
            for p in range(1, G):
                total = total + unpack(y_rx.at[j, p, q])
            fin[j, q] = total
            at = pl.ds(pl.multiple_of(j * dk, 8), dk), pl.ds(pl.multiple_of((q + B0 * h) * bw, 128), bw)
            remote(fin.at[j, q], out_b.at[at], f_recv, sib).start()
            out_b[at] = total
        own(q, lambda: pl.when(cs == c)(go))

    def bra_e():
        for x, n in ((1, B0), (0, B1)):
            pl.when(h == x)(lambda: recv(fin.at[:, pl.ds(0, n)], f_recv))

    others = [(c + o) % C for o in range(1, C)]

    def bra_forward():
        for o, p in enumerate(others):
            recv(bbuf.at[p, h], b_recv.at[0, o])
            remote(bbuf.at[p, h], bbuf.at[p, h], b_recv.at[1, o], sib).start()
            sent(None, bbuf.at[p, h])

    def ket_others():
        for o, p in enumerate(others):
            recv(bbuf.at[p, 1 - h], b_recv.at[1, o])
            ket_block(p)
            ket_ends(p, range(SP))

    def take_dot(i, lo, hi, *more):
        for u in range(lo, hi):
            for k in (i, *more):
                ket_take(k, u)
        bra_dot(i, lo, hi)

    mid = KP // 2

    def start_edge():
        ket_ends(c, range(SP), False)
        bra_dot(0, 0, KP)
        take_dot(1, 0, mid)
        take_dot(1, mid, KP)
        bra_forward()
        bra_b(0)
        ket_others()
        ket_ends(c, [SP - 1], True)
        bra_b(1)
        for i in range(2, R):
            if i > 2:
                bra_b(i - 1)
                for q in range(max(B0, B1)):
                    bra_c(i - 3, q)
            take_dot(i, 0, mid)
            take_dot(i, mid, KP - 1)
            take_dot(i, KP - 1, KP)
        for q in range(max(B0, B1)):
            bra_c(R - 2, q)
        bra_b(R - 1)
        for q in range(max(B0, B1)):
            bra_c(R - 3, q)
        return R - 1

    def start_inside():
        bra_dot(0, 0, KP)
        take_dot(1, 0, mid, 2)
        take_dot(1, mid, KP, 2)
        bra_b(0)
        bra_dot(2, 0, KP)
        bra_forward()
        take_dot(3, 0, mid)
        bra_b(1)
        take_dot(3, mid, KP)
        ket_others()
        bra_b(2)
        for i in range(4, R):
            take_dot(i, 0, KP)
            bra_b(i - 1)
        return 0

    def finish(kind, done):
        tail = [] if kind == "edge" else [(12.1, bra_b, (R - 1,))]
        for late in (False, True):
            lag = HOPS[late]
            if kind == "edge":
                steps = range(lag * (R - 2), lag * (R - 2) + SP)
            else:
                steps = range(max((R - hop) * SP + lag * (hop - 1) for hop in range(1, R - 1)))
            for p in steps:
                tail.append(((13.5 if late else 8.5) + 1.05 * p, flow, (late, p)))
        if kind == "edge":
            when_bra = {0: (12.9, 16.5, 1.0), 1: (15.5, 19.2, 1.0), 2: (15.6, 22.3, 0.1), 3: (19.0, 22.5, 1.05)}
        else:
            when_bra = {0: (12.4, 16.5, 0.6), 1: (13.4, 17.1, 1.0), 2: (16.0, 20.7, 0.5), 3: (16.0, 20.1, 1.0)}
        for i in range(R):
            col_at, depth_at, step = when_bra.get(i, (19.0 + 4 * (i - 3), 22.5 + 4 * (i - 3), 1.05))
            for q in range(max(B0, B1)):
                if i >= done:
                    tail.append((col_at + step * q, bra_c, (i, q)))
                tail.append((depth_at + step * q, bra_d, (i, q)))
        tail.sort(key=lambda x: x[0])
        first_done = last_done = False
        for at, fn, args in tail:
            if at > 19 and not first_done:
                flush("first")
                first_done = True
            if at > 23.6 and not last_done:
                flush("last")
                last_done = True
            fn(*args)
        bra_e()
        for u in range(SP):
            out_k[:, u * sw:(u + 1) * sw] = kpart[r, u]
        pending["last"].clear()
        for t in range(R):
            sent(t != r, k_tx.at[t], "last")
        for j in range(per):
            for o in range(1, G):
                sent_own(None, y_rx.at[j, g], "last")
            sent_own(None, fin.at[j], "last")
        flush("last")

    ket_block(c)
    front = list(pending["first"])

    def run(kind):
        pending["first"], pending["last"] = list(front), []
        finish(kind, start_edge() if kind == "edge" else start_inside())

    pl.when(near == 0)(lambda: run("edge"))
    pl.when(near > 0)(lambda: run("inside"))


def store(bra_t, ket_t, bra, ket, turned, sem):
    kets = pltpu.make_async_copy(ket_t, ket, sem.at[0])
    kets.start()
    size = turned.shape[0] // STORES
    copies = []
    for i in range(STORES):
        at = pl.ds(i * size, size)
        turned[at] = bra_t[:, at].T
        copies.append(pltpu.make_async_copy(turned.at[at], bra.at[at], sem.at[1 + i]))
        copies[-1].start()
    for one in [kets, *copies]:
        one.wait()


def body(sizes, eri_tiles, screen, density_bra, density_ket):
    R, C, Dp = sizes
    A, B, PS, _ = eri_tiles.shape
    rows, cols = A * PS, B * PS
    db, dk = density_bra.shape[1], density_ket.shape[1]
    per, G, half = R // C, Dp // 2, rows // 2
    DMA = pltpu.SemaphoreType.DMA
    hbm = pl.BlockSpec(memory_space=pltpu.HBM)
    vm = pl.BlockSpec(memory_space=pltpu.VMEM)
    piece, coded, most = (dk, rows // BP), (dk, rows // BP * 3 // 2), max(B0, BP - B0)
    out_b, out_k = pl.pallas_call(
        functools.partial(kernel, sizes),
        out_shape=(jax.ShapeDtypeStruct((db, rows), F32), jax.ShapeDtypeStruct((dk, cols), F32)),
        in_specs=[hbm, hbm, hbm, hbm],
        out_specs=(vm, vm),
        scratch_shapes=[
            pltpu.SMEM((B, A), jnp.int32),
            pltpu.VMEM((A, B, PS, PS), BF16),
            pltpu.VMEM((rows, cols), BF16),
            pltpu.VMEM((R, KP, dk, cols // KP), BF16),
            pltpu.VMEM((C, 2, half, db), BF16),
            pltpu.VMEM((R, SP, dk, cols // SP), F32),
            pltpu.VMEM((R, SP, dk, cols // SP * 3 // 2), BF16),
            pltpu.VMEM((2, R, SP, dk, cols // SP * 3 // 2), BF16),
            pltpu.VMEM((R, BP, *piece), F32),
            pltpu.VMEM((R, most, *piece), F32),
            pltpu.VMEM((R, most, *coded), BF16),
            pltpu.VMEM((C, per, most, *coded), BF16),
            pltpu.VMEM((per, G, most, *coded), BF16),
            pltpu.VMEM((per, most, *piece), F32),
            DMA((4,)), DMA, DMA((R, KP)), DMA((2, C - 1)), DMA((R + 1, SP)),
            DMA((R, most)), DMA((C - 1, per, most)), DMA((per, G - 1, most)), DMA,
        ],
        compiler_params=pltpu.CompilerParams(
            collective_id=0, has_side_effects=True, vmem_limit_bytes=28 * 1024 * 1024),
    )(*(pltpu.with_memory_space_constraint(x, pltpu.HBM) for x in (eri_tiles, screen.T, density_bra, density_ket.T)))
    bra, ket = pl.pallas_call(
        store,
        out_shape=(jax.ShapeDtypeStruct((rows, db), F32), jax.ShapeDtypeStruct((dk, cols), F32)),
        in_specs=[vm, vm],
        out_specs=(hbm, hbm),
        scratch_shapes=[pltpu.VMEM((rows, db), F32), DMA((1 + STORES,))],
        compiler_params=pltpu.CompilerParams(vmem_limit_bytes=4 * 1024 * 1024),
    )(out_b, out_k)
    return bra, ket.T


def solution(mesh):
    sizes = (mesh.shape["row"], mesh.shape["col"], mesh.shape["depth"])
    return jax.shard_map(
        functools.partial(body, sizes),
        mesh=mesh,
        in_specs=(
            P("row", ("col", "depth"), None, None),
            P("row", ("col", "depth")),
            P("row", "col"),
            P(("col", "depth"), "row"),
        ),
        out_specs=(P("row", "col"), P(("col", "depth"), "row")),
        check_vma=False,
    )
```
